32 devices in a mesh: rep: 4 (over y, x), tile: 8 (over z, core).
Axes of the slice: x: 2, y: 2, z: 4, core: 2. Of those that a mesh axis runs over, the one named last changes fastest.
Arguments:
- feature_tiles: bfloat16 [64, 16, 128, 128], P(('rep', 'tile')), parts along dimension 0, may hold values from -6 to 6
- neighbours: int32 [64, 4], P('rep'), parts along dimension 0, may hold values from -1 to 15, as said below
- valid_rows: int32 [64], P('rep'), parts along dimension 0, may hold values from 4 to 16, as said below
- tile_image: int32 [64], P('rep'), parts along dimension 0, may hold values from 0 to 7, as said below
- gain_one: float32 [128], replicated, may hold values from 0.1 to 1.9
- shift_one: float32 [128], replicated, may hold values from -3 to 3
- kernel_one: bfloat16 [3, 3, 128, 128], replicated, may hold values from -0.1875 to 0.1875
- offset_one: float32 [128], replicated, may hold values from -3 to 3
- gain_two: float32 [128], replicated, may hold values from 0.1 to 1.9
- shift_two: float32 [128], replicated, may hold values from -3 to 3
- kernel_two: bfloat16 [3, 3, 128, 128], replicated, may hold values from -0.1875 to 0.1875
- offset_two: float32 [128], replicated, may hold values from -3 to 3
Outputs:
- block_out: bfloat16 [64, 16, 128, 128], P(('rep', 'tile')), parts along dimension 0
The draws below stay inside these ranges and needn't reach their ends.
There are 4 independent parts, one for each index of `rep`. The reference program is written for one: setup_inputs(seed, part) draws one part's arguments, and reference() takes and returns one part's arrays. A program takes and returns all parts, laid end to end along the dimension named above; an argument that names none is the same for every part. Nothing has to cross between parts.
Inputs may be any that keep to these rules, and one draw needn't show every extreme that they name: Each image is a rectangle of tiles; neighbours name the adjacent tile of the same image in that direction, or -1 at the image's border. `valid_rows`: only tiles in the bottom row of tiles of an image have fewer than 16 rows; all tiles of that row have the same count. `tile_image`: image numbers need not be consecutive; some may be unused.
All inputs are finite; a program needn't handle non-finite values.
Results may differ from the reference program's by a relative error of at most 0.0075.
Values may be sent and summed in bfloat16 or wider, within the bound.
No kernel may reach another device: no remote copies, remote signals or barrier semaphores. Data moves between devices by JAX's collectives and lax.ppermute only.
A program may use at most 64 MiB of HBM per device.

```python
import jax
import jax.numpy as jnp
from jax import lax

C = 128
G = 32
TH = 16
TW = 128
NT = 16
IMAGES = 8


def layout(key):
    folded = jax.random.fold_in(key, 7)
    key_start, key_cut, key_rows, key_order = jax.random.split(folded, 4)
    band_rows = NT // 4
    starts = jax.random.randint(key_start, (band_rows,), 0, 2).astype(jnp.int32).at[0].set(1)
    band_of = jnp.cumsum(starts) - 1
    cut_col = jax.random.randint(key_cut, (band_rows,), 1, 5).astype(jnp.int32)[band_of]
    column = jnp.arange(4, dtype=jnp.int32)
    image_of = band_of[:, None] * 2 + (column[None, :] >= cut_col[:, None]).astype(jnp.int32)
    top_image = jnp.max(image_of)
    image_of = jnp.where(image_of == top_image, NT // 2 - 1, image_of).astype(jnp.int32)
    ending = jnp.concatenate([starts[1:], jnp.ones((1,), jnp.int32)])
    drawn_rows = jax.random.randint(key_rows, (band_rows,), TH // 4, TH + 1).astype(jnp.int32)[band_of]
    row_count = jnp.where(ending == 1, drawn_rows, TH)
    row_grid = jnp.broadcast_to(row_count[:, None], (band_rows, 4))
    canonical = jnp.arange(band_rows, dtype=jnp.int32)[:, None] * 4 + column[None, :]
    upper_slot = jnp.where(starts[:, None] == 0, canonical - 4, -1)
    lower_slot = jnp.where(ending[:, None] == 0, canonical + 4, -1)
    left_image = jnp.concatenate([jnp.full((band_rows, 1), -1, jnp.int32), image_of[:, :-1]], axis=1)
    right_image = jnp.concatenate([image_of[:, 1:], jnp.full((band_rows, 1), -1, jnp.int32)], axis=1)
    left_slot = jnp.where(left_image == image_of, canonical - 1, -1)
    right_slot = jnp.where(right_image == image_of, canonical + 1, -1)
    order_map = jax.random.permutation(key_order, NT).astype(jnp.int32)
    linked = jnp.stack([upper_slot, lower_slot, left_slot, right_slot], axis=-1).reshape(NT, 4)
    linked = jnp.where(linked >= 0, order_map[jnp.maximum(linked, 0)], -1)
    neighbour_table = jnp.zeros((NT, 4), jnp.int32).at[order_map].set(linked)
    rows_table = jnp.zeros((NT,), jnp.int32).at[order_map].set(row_grid.reshape(NT))
    image_table = jnp.zeros((NT,), jnp.int32).at[order_map].set(image_of.reshape(NT))
    return (neighbour_table, rows_table, image_table)


def draw_neighbours(key, part):
    return layout(key)[0]


def draw_valid_rows(key, part):
    return layout(key)[1]


def draw_tile_image(key, part):
    return layout(key)[2]


def steps_of(rng, extent, shards, smallest, top_value):
    gain, own = 1.0, jax.random.fold_in(rng, 6)
    for position, parts in shards:
        heights = jnp.exp(jax.random.uniform(jax.random.fold_in(own, position), (parts,), jnp.float32, smallest / len(shards), top_value / len(shards)))
        gain = gain * jnp.repeat(heights, extent[position] // parts).reshape([-1 if axis == position else 1 for axis in range(len(extent))])
    return gain


def normal_values(stream_key, shape, spread, limit, pieces=(), kind=jnp.bfloat16):
    values = jax.random.normal(stream_key, shape, jnp.float32) * spread
    if len(pieces) > 0:
        values = steps_of(stream_key, shape, pieces, -0.22, 0.18) * values
    return jnp.clip(values, min=-limit, max=limit).astype(kind)


def setup_inputs(seed: int = 0, part: int = 0) -> dict:
    splits = jax.random.split(jax.random.key(seed), 13)
    part_keys = jax.random.split(jax.random.fold_in(splits[12], part), 13)
    return {
        "feature_tiles": normal_values(part_keys[0], (NT, TH, TW, C), 1.0, 6.0, ((0, 8),)),
        "neighbours": draw_neighbours(jax.random.fold_in(jax.random.fold_in(splits[12], part), 71), part),
        "valid_rows": draw_valid_rows(jax.random.fold_in(jax.random.fold_in(splits[12], part), 71), part),
        "tile_image": draw_tile_image(jax.random.fold_in(jax.random.fold_in(splits[12], part), 71), part),
        "gain_one": jnp.clip(1.0 + 0.18 * jax.random.normal(splits[4], (C,), jnp.float32), 0.1, 1.9),
        "shift_one": normal_values(splits[5], (C,), 0.5, 3.0, (), jnp.float32),
        "kernel_one": normal_values(splits[6], (3, 3, C, C), (9 * C) ** -0.5, 0.1875),
        "offset_one": normal_values(splits[7], (C,), 0.5, 3.0, (), jnp.float32),
        "gain_two": jnp.clip(1.0 + 0.18 * jax.random.normal(splits[8], (C,), jnp.float32), 0.1, 1.9),
        "shift_two": normal_values(splits[9], (C,), 0.5, 3.0, (), jnp.float32),
        "kernel_two": normal_values(splits[10], (3, 3, C, C), (9 * C) ** -0.5, 0.1875),
        "offset_two": normal_values(splits[11], (C,), 0.5, 3.0, (), jnp.float32),
    }


epsilon = 1e-06

def pick(source, indices):
    clamped = jnp.maximum(indices, 0).astype(jnp.int32)
    fetched = jnp.take(source, clamped, axis=0)
    present = (indices >= 0).reshape(indices.shape + (1,) * (fetched.ndim - 1))
    return jnp.where(present, fetched, jnp.zeros_like(fetched))

def widen(feature, neighbours):
    left_col = pick(feature[:, :, -1, :], neighbours[:, 2])
    right_col = pick(feature[:, :, 0, :], neighbours[:, 3])
    widened = jnp.concatenate([left_col[:, :, None], feature, right_col[:, :, None]], axis=2)
    upper_row = pick(widened[:, -1], neighbours[:, 0])
    lower_row = pick(widened[:, 0], neighbours[:, 1])
    return jnp.concatenate([upper_row[:, None], widened, lower_row[:, None]], axis=1)

def convolve(padded, kernel, offset):
    tile_count, rows_pad, cols_pad, channels = padded.shape
    tile_rows, tile_cols = (rows_pad - 2, cols_pad - 2)
    summed = jnp.zeros((tile_count * tile_rows * tile_cols, kernel.shape[3]), jnp.float32)
    for row_off in range(3):
        for col_off in range(3):
            window = padded[:, row_off:row_off + tile_rows, col_off:col_off + tile_cols, :].reshape(-1, channels)
            summed = summed + jnp.dot(window, kernel[row_off, col_off], preferred_element_type=jnp.float32)
    return summed.reshape(tile_count, tile_rows, tile_cols, -1) + offset

def group_sums(per_tile, member, groups):
    images = jnp.dot(member.T, per_tile, precision=lax.Precision.HIGHEST)
    return images.reshape(images.shape[0], groups, -1).sum(axis=2)

def to_tiles(per_group, member, group_width):
    per_channel = jnp.repeat(per_group, group_width, axis=1)
    return jnp.dot(member, per_channel, precision=lax.Precision.HIGHEST)

def normalize(feature, row_mask, member, counts, gain_vec, shift_vec):
    group_width = feature.shape[3] // G
    mask_full = row_mask[:, :, None, None]
    masked = feature * mask_full
    means = group_sums(lax.optimization_barrier(jnp.sum(masked, axis=(1, 2))), member, G) / counts
    centred = (feature - to_tiles(means, member, group_width)[:, None, None, :]) * mask_full
    variance = group_sums(lax.optimization_barrier(jnp.sum(centred * centred, axis=(1, 2))), member, G) / counts
    inverse = lax.rsqrt(to_tiles(variance, member, group_width) + epsilon)
    normed = centred * inverse[:, None, None, :] * gain_vec + shift_vec
    return (jax.nn.silu(normed) * mask_full).astype(jnp.bfloat16)

def reference(feature_tiles, neighbours, valid_rows, tile_image, gain_one, shift_one, kernel_one, offset_one, gain_two, shift_two, kernel_two, offset_two):
    row_mask = (jnp.arange(TH)[None, :] < valid_rows[:, None]).astype(jnp.float32)
    mask_full = row_mask[:, :, None, None]
    member = (tile_image[:, None] == jnp.arange(IMAGES)[None, :]).astype(jnp.float32)
    pixels = (valid_rows * TW).astype(jnp.float32)
    counts = jnp.maximum(jnp.dot(member.T, pixels[:, None], precision=lax.Precision.HIGHEST) * (C // G), 1.0)
    inputs = feature_tiles.astype(jnp.float32) * mask_full
    first_act = normalize(inputs, row_mask, member, counts, gain_one, shift_one)
    hidden = (convolve(widen(first_act, neighbours), kernel_one, offset_one) * mask_full).astype(jnp.bfloat16)
    second_act = normalize(hidden.astype(jnp.float32), row_mask, member, counts, gain_two, shift_two)
    mixed_out = convolve(widen(second_act, neighbours), kernel_two, offset_two)
    return ((inputs + mixed_out) * mask_full).astype(jnp.bfloat16)
```

```python
import functools

import jax
import jax.numpy as jnp
from jax import lax
from jax.experimental import pallas as pl
from jax.experimental.pallas import tpu as pltpu
from jax.sharding import PartitionSpec as P

G = 32
AXIS = "tile"
epsilon = 1e-06
f32 = jnp.float32
bf16 = jnp.bfloat16


VMEM = pl.BlockSpec(memory_space=pltpu.VMEM)
SMEM = pl.BlockSpec(memory_space=pltpu.SMEM)


def round_up(value, step):
    return -(-value // step) * step


class Plan:
    def __init__(self, size, count, rows, cols, channels):
        self.size, self.count, self.rows, self.cols, self.channels = size, count, rows, cols, channels
        chips = size // 2
        fits = size % 2 == 0 and chips & (chips - 1) == 0 and cols % (16 * max(chips, 1)) == 0
        self.chunks = chips if fits and chips > 1 else 1
        self.width = cols // self.chunks
        self.stat_rows = round_up(6 * count, 16)
        self.row_base = self.stat_rows
        self.col_base = self.row_base + 2 * count * self.width
        self.buf_rows = self.col_base + 2 * count * rows
        self.slots = size

    def place(self):
        index = lax.axis_index(AXIS)
        return lax.div(index, 2), lax.rem(index, 2)

    def chunk(self, k):
        return lax.bitwise_xor(self.place()[0], k) if self.chunks > 1 else 0

    def slot_of(self, device):
        if self.chunks == 1:
            return device
        chip, core = self.place()
        other = lax.bitwise_xor(lax.rem(device, 2), core)
        return other * self.chunks + lax.bitwise_xor(lax.div(device, 2), chip)

    def device_of(self, slot):
        if self.chunks == 1:
            return slot
        chip, core = self.place()
        return lax.bitwise_xor(chip, slot % self.chunks) * 2 + lax.bitwise_xor(core, slot // self.chunks)

    def target(self, k):
        if self.chunks == 1:
            return lax.axis_index(AXIS)
        chip, core = self.place()
        return lax.bitwise_xor(chip, k) * 2 + core


def split_three(values):
    high = values.astype(bf16)
    rest = values - high.astype(f32)
    middle = rest.astype(bf16)
    low = (rest - middle.astype(f32)).astype(bf16)
    return high.astype(f32), middle.astype(f32), low.astype(f32)


def fold_rows(values):
    return values.reshape(-1, 8, values.shape[-1]).sum(axis=0)


def fill_buffers(plan, source_ref, own_rows, buf_refs):
    sums, squares = [], []
    for tile in range(plan.count):
        valid = own_rows[tile]

        def total(row, acc):
            part = fold_rows(source_ref[tile, row].astype(f32))
            return acc + jnp.where(row < valid, part, 0.0)

        acc = jnp.zeros((8, plan.channels), f32)
        for row in range(plan.rows):
            acc = total(row, acc)
        tile_sum = jnp.sum(acc, axis=0, keepdims=True)
        pixels = jnp.maximum(valid * plan.cols, 1).astype(f32)
        tile_mean = tile_sum / pixels
        acc = jnp.zeros((8, plan.channels), f32)
        for row in range(plan.rows):
            offset = source_ref[tile, row].astype(f32) - tile_mean
            acc = acc + jnp.where(row < valid, fold_rows(offset * offset), 0.0)
        sums.append(tile_sum)
        squares.append(jnp.sum(acc, axis=0, keepdims=True))
    parts = split_three(jnp.concatenate(sums + squares, axis=0))
    padding = plan.stat_rows - 6 * plan.count
    pieces = list(parts) + ([jnp.zeros((padding, plan.channels), f32)] if padding else [])
    stats = jnp.concatenate(pieces, axis=0).astype(bf16)
    columns = []
    for tile in range(plan.count):
        for column in (0, plan.cols - 1):
            picked = [source_ref[tile, row, column : column + 1, :].astype(f32) for row in range(plan.rows)]
            columns.append(jnp.concatenate(picked, axis=0).astype(bf16))
    for k in range(plan.chunks):
        buf_refs[k][0 : plan.stat_rows, :] = stats
        start = plan.chunk(k) * plan.width
        if plan.chunks > 1:
            start = pl.multiple_of(start, 16)
        for tile in range(plan.count):
            for edge, row in enumerate((0, plan.rows - 1)):
                at = plan.row_base + (2 * tile + edge) * plan.width
                buf_refs[k][at : at + plan.width, :] = source_ref[tile, row, pl.ds(start, plan.width), :]
        for place, column in enumerate(columns):
            at = plan.col_base + place * plan.rows
            buf_refs[k][at : at + plan.rows, :] = column


def own_values(plan, ref):
    first = lax.axis_index(AXIS) * plan.count
    return [ref[first + tile] for tile in range(plan.count)]


def gather_kernel(plan, rows_ref, x_ref, *buf_refs):
    fill_buffers(plan, x_ref, own_values(plan, rows_ref), buf_refs)


def group_total(values, group_width):
    lanes = values.shape[-1]
    lane = lax.broadcasted_iota(jnp.int32, values.shape, 1)
    step = 1
    while step < group_width:
        ahead = pltpu.roll(values, lanes - step, axis=1)
        behind = pltpu.roll(values, step, axis=1)
        values = values + jnp.where(lax.bitwise_and(lane, step) == 0, ahead, behind)
        step *= 2
    return values


def route_kernel(plan, links_ref, rows_ref, image_ref, *refs):
    inputs = plan.slots if plan.chunks > 1 else 1
    bufs, (norm_ref, side_ref), send_refs, held = (
        refs[:inputs],
        refs[inputs : inputs + 2],
        refs[inputs + 2 : -1],
        refs[-1],
    )
    if plan.chunks > 1:
        for slot in range(plan.slots):
            held[slot] = bufs[slot][...]
    else:
        held = bufs[0]
    count, rows, width = plan.count, plan.rows, plan.width

    def locate(tile):
        tile = jnp.maximum(tile, 0)
        return plan.slot_of(lax.div(tile, count)), lax.rem(tile, count)

    def edge_row(tile, edge):
        slot, local = locate(tile)
        at = pl.multiple_of(plan.row_base + (2 * local + edge) * width, 16)
        return held[slot, pl.ds(at, width), :]

    def edge_col(tile, edge):
        slot, local = locate(tile)
        at = pl.multiple_of(plan.col_base + (2 * local + edge) * rows, 16)
        return held[slot, pl.ds(at, rows), :]

    def across(tile, column):
        return links_ref[jnp.maximum(tile, 0) * 4 + column]

    for k in range(plan.chunks):
        first = plan.target(k) * count
        for tile in range(count):
            for edge in range(2):
                at = (2 * tile + edge) * width
                wanted = links_ref[(first + tile) * 4 + edge]
                send_refs[k][at : at + width, :] = edge_row(wanted, 1 - edge)

    first = lax.axis_index(AXIS) * count
    for tile in range(count):
        at = tile * 3 * rows
        link = [links_ref[(first + tile) * 4 + column] for column in range(4)]
        side_ref[at : at + rows, :] = edge_col(link[2], 1)
        side_ref[at + rows : at + 2 * rows, :] = edge_col(link[3], 0)
        corners = [
            edge_col(across(link[0], 2), 1)[rows - 1 : rows].astype(f32),
            edge_col(across(link[0], 3), 0)[rows - 1 : rows].astype(f32),
            edge_col(across(link[1], 2), 1)[0:1].astype(f32),
            edge_col(across(link[1], 3), 0)[0:1].astype(f32),
        ]
        corners.append(jnp.zeros((rows - 4, plan.channels), f32))
        side_ref[at + 2 * rows : at + 3 * rows, :] = jnp.concatenate(corners, axis=0).astype(bf16)

    group_width = plan.channels // G
    partial = []
    for slot in range(plan.slots):
        raw = held[slot, 0 : plan.stat_rows, :].astype(f32)
        span = 2 * count
        partial.append(raw[0:span] + raw[span : 2 * span] + raw[2 * span : 3 * span])
    means, inverses = [], []
    for tile in range(count):
        image = image_ref[first + tile]
        weights, pixels = [], []
        area = jnp.int32(0)
        for slot in range(plan.slots):
            base = plan.device_of(slot) * count
            for other in range(count):
                same = image_ref[base + other] == image
                weights.append(jnp.where(same, 1.0, 0.0).astype(f32))
                amount = rows_ref[base + other] * plan.cols
                pixels.append(amount.astype(f32))
                area = area + jnp.where(same, amount, 0)
        total = jnp.zeros((1, plan.channels), f32)
        for slot in range(plan.slots):
            for other in range(count):
                total = total + weights[slot * count + other] * partial[slot][other : other + 1]
        amount = jnp.maximum(area * group_width, 1).astype(f32)
        mean = group_total(jnp.broadcast_to(total, (8, plan.channels)), group_width)[0:1] / amount
        total = jnp.zeros((1, plan.channels), f32)
        for slot in range(plan.slots):
            for other in range(count):
                place = slot * count + other
                apart = partial[slot][other : other + 1] / pixels[place] - mean
                spread = partial[slot][count + other : count + other + 1] + pixels[place] * apart * apart
                total = total + weights[place] * spread
        variance = group_total(jnp.broadcast_to(total, (8, plan.channels)), group_width)[0:1] / amount
        means.append(mean)
        inverses.append(lax.rsqrt(variance + epsilon))
    norm_ref[0 : 2 * count, :] = jnp.concatenate(means + inverses, axis=0)


def conv_kernel(plan, last, links_ref, rows_ref, image_ref, *refs):
    del image_ref
    x_ref, norm_ref, side_ref, gain_ref, shift_ref, offset_ref, weight_ref = refs[:7]
    refs = refs[7:]
    residual_ref = None
    if last:
        residual_ref, refs = refs[0], refs[1:]
    halo_refs, refs = refs[: plan.chunks], refs[plan.chunks :]
    out_ref, refs = refs[0], refs[1:]
    if last:
        buf_refs, (wide, halo) = (), refs
    else:
        buf_refs, (wide, halo) = refs[: plan.chunks], refs[plan.chunks :]
    count, rows, cols, channels = plan.count, plan.rows, plan.cols, plan.channels
    first = lax.axis_index(AXIS) * count
    own_rows = own_values(plan, rows_ref)

    for k in range(plan.chunks):
        start = plan.chunk(k) * plan.width
        if plan.chunks > 1:
            start = pl.multiple_of(start, 16)
        for place in range(2 * count):
            at = place * plan.width
            halo[place, pl.ds(start, plan.width), :] = halo_refs[k][at : at + plan.width, :]

    pixel = lax.broadcasted_iota(jnp.int32, (cols, channels), 0)
    gain = gain_ref[...] * 0.5
    shift = shift_ref[...] * 0.5
    offset = offset_ref[...]

    def across(tile, column):
        return jnp.where(tile >= 0, links_ref[jnp.maximum(tile, 0) * 4 + column], -1)

    for tile in range(count):
        valid = own_rows[tile]
        mean = norm_ref[tile : tile + 1, :]
        scale = norm_ref[count + tile : count + tile + 1, :] * gain
        link = [links_ref[(first + tile) * 4 + column] for column in range(4)]

        def activate(values):
            half = (values.astype(f32) - mean) * scale + shift
            return half + half * jnp.tanh(half)

        at = tile * 3 * rows
        left = jnp.where(link[2] >= 0, activate(side_ref[at : at + rows, :]), 0.0)
        right = jnp.where(link[3] >= 0, activate(side_ref[at + rows : at + 2 * rows, :]), 0.0)
        corner = activate(side_ref[at + 2 * rows : at + 3 * rows, :])
        corner = [
            jnp.where(across(link[place // 2], 2 + place % 2) >= 0, corner[place : place + 1], 0.0)
            for place in range(4)
        ]
        for padded in range(rows + 2):
            row = padded - 1
            if row == -1 or row == rows:
                edge = 0 if row == -1 else 1
                act = jnp.where(link[edge] >= 0, activate(halo[2 * tile + edge]), 0.0)
                before, after = corner[2 * edge], corner[2 * edge + 1]
            else:
                act = jnp.where(row < valid, activate(x_ref[tile, row]), 0.0)
                before = jnp.where(row < valid, left[row : row + 1], 0.0)
                after = jnp.where(row < valid, right[row : row + 1], 0.0)
            lane = (padded % 2) * 3 * channels
            back = jnp.where(pixel == 0, before, pltpu.roll(act, 1, axis=0))
            ahead = jnp.where(pixel == cols - 1, after, pltpu.roll(act, cols - 1, axis=0))
            for tap, values in enumerate((back, act, ahead)):
                at_lane = lane + tap * channels
                wide[tile, padded // 2, :, at_lane : at_lane + channels] = values.astype(bf16)

        pairs = rows // 2
        depth = 6 * channels
        upper = wide[tile, 0:pairs].reshape(pairs * cols, depth)
        lower = wide[tile, 1 : pairs + 1].reshape(pairs * cols, depth)
        summed = jnp.dot(upper, weight_ref[0:depth, :], preferred_element_type=f32)
        summed = summed + jnp.dot(lower, weight_ref[depth : 2 * depth, :], preferred_element_type=f32)
        for row in range(rows):
            part = summed[(row // 2) * cols : (row // 2 + 1) * cols, (row % 2) * channels : (row % 2 + 1) * channels]
            part = part + offset
            if last:
                part = part + residual_ref[tile, row].astype(f32)
            out_ref[tile, row] = jnp.where(row < valid, part, 0.0).astype(bf16)

    if not last:
        fill_buffers(plan, out_ref, own_rows, buf_refs)


def paired_weights(kernel):
    upper = jnp.pad(kernel, ((0, 1), (0, 0), (0, 0), (0, 0)))
    lower = jnp.pad(kernel, ((1, 0), (0, 0), (0, 0), (0, 0)))
    both = jnp.concatenate([upper, lower], axis=-1)
    return both.reshape(-1, both.shape[-1])


def shards(
    feature_tiles,
    neighbours,
    valid_rows,
    tile_image,
    gain_one,
    shift_one,
    kernel_one,
    offset_one,
    gain_two,
    shift_two,
    kernel_two,
    offset_two,
    *,
    size,
):
    count, rows, cols, channels = feature_tiles.shape
    plan = Plan(size, count, rows, cols, channels)
    links = neighbours.reshape(-1)
    scalars = (links, valid_rows, tile_image)
    buf_shape = [jax.ShapeDtypeStruct((plan.buf_rows, channels), bf16)] * plan.chunks
    limit = 24 * 1024 * 1024
    params = pltpu.CompilerParams(vmem_limit_bytes=limit)

    def swap(array, distance):
        return lax.ppermute(array, AXIS, [(i, i ^ distance) for i in range(size)])

    def exchange(bufs):
        if plan.chunks == 1:
            return [lax.all_gather(bufs[0], AXIS)]
        own = [bufs[0]] + [swap(bufs[k], 2 * k) for k in range(1, plan.chunks)]
        return own + [swap(array, 1) for array in own]

    def route(arrays):
        scratch = (plan.slots, plan.buf_rows, channels) if plan.chunks > 1 else (1, 16, channels)
        norm, side, *send = pl.pallas_call(
            functools.partial(route_kernel, plan),
            out_shape=[
                jax.ShapeDtypeStruct((round_up(2 * count, 8), channels), f32),
                jax.ShapeDtypeStruct((3 * rows * count, channels), bf16),
            ]
            + [jax.ShapeDtypeStruct((2 * count * plan.width, channels), bf16)] * plan.chunks,
            in_specs=[SMEM] * 3 + [VMEM] * len(arrays),
            out_specs=[VMEM] * (2 + plan.chunks),
            scratch_shapes=[pltpu.VMEM(scratch, bf16)],
            compiler_params=params,
            name="route",
        )(*scalars, *arrays)
        halo = [send[0]] + [swap(send[k], 2 * k) for k in range(1, plan.chunks)]
        return norm, side, halo

    def stage(last, source, arrays, gain, shift, kernel, offset):
        norm, side, halo = route(arrays)
        operands = [source, norm, side, gain[None], shift[None], offset[None], paired_weights(kernel)]
        if last:
            operands.append(feature_tiles)
        operands += halo
        out_shape = [jax.ShapeDtypeStruct(feature_tiles.shape, bf16)] + ([] if last else buf_shape)
        flops = 2 * count * rows * cols * 9 * channels * channels
        return pl.pallas_call(
            functools.partial(conv_kernel, plan, last),
            out_shape=out_shape,
            in_specs=[SMEM] * 3 + [VMEM] * len(operands),
            out_specs=[VMEM] * len(out_shape),
            scratch_shapes=[
                pltpu.VMEM((count, rows // 2 + 1, cols, 6 * channels), bf16),
                pltpu.VMEM((2 * count, cols, channels), bf16),
            ],
            compiler_params=params,
            cost_estimate=pl.CostEstimate(flops=flops, bytes_accessed=3 * feature_tiles.size, transcendentals=0),
            name="conv_last" if last else "conv_first",
        )(*scalars, *operands)

    bufs = pl.pallas_call(
        functools.partial(gather_kernel, plan),
        out_shape=buf_shape,
        in_specs=[SMEM, VMEM],
        out_specs=[VMEM] * plan.chunks,
        compiler_params=params,
        name="edges",
    )(valid_rows, feature_tiles)
    hidden, *bufs = stage(False, feature_tiles, exchange(bufs), gain_one, shift_one, kernel_one, offset_one)
    return stage(True, hidden, exchange(bufs), gain_two, shift_two, kernel_two, offset_two)[0]


def solution(mesh):
    in_specs = (
        P(("rep", "tile"), None, None, None),
        P("rep", None),
        P("rep"),
        P("rep"),
        P(),
        P(),
        P(),
        P(),
        P(),
        P(),
        P(),
        P(),
    )
    out_specs = P(("rep", "tile"), None, None, None)
    body = functools.partial(shards, size=mesh.shape[AXIS])
    return jax.shard_map(body, mesh=mesh, in_specs=in_specs, out_specs=out_specs, check_vma=False)
```

```python
import functools

import jax
import jax.numpy as jnp
from jax import lax
from jax.experimental import pallas as pl
from jax.experimental.pallas import tpu as pltpu
from jax.sharding import PartitionSpec as P


G = 32
AXIS = "tile"
epsilon = 1e-06
f32 = jnp.float32
bf16 = jnp.bfloat16


VMEM = pl.BlockSpec(memory_space=pltpu.VMEM)
SMEM = pl.BlockSpec(memory_space=pltpu.SMEM)
HBM = pl.BlockSpec(memory_space=pltpu.HBM)


def round_up(value, step):
    return -(-value // step) * step


class Plan:
    def __init__(self, size, count, rows, cols, channels):
        self.size, self.count, self.rows, self.cols, self.channels = size, count, rows, cols, channels
        chips = size // 2
        fits = size % 2 == 0 and chips & (chips - 1) == 0 and cols % (16 * max(chips, 1)) == 0
        self.chunks = chips if fits and chips > 1 else 1
        self.width = cols // self.chunks
        self.stat_rows = round_up(6 * count, 16)
        self.row_base = self.stat_rows
        self.col_base = self.row_base + 2 * count * self.width
        self.buf_rows = self.col_base + 2 * count * rows
        self.slots = size

    def place(self):
        index = lax.axis_index(AXIS)
        return lax.div(index, 2), lax.rem(index, 2)

    def chunk(self, k):
        return lax.bitwise_xor(self.place()[0], k) if self.chunks > 1 else 0

    def slot_of(self, device):
        if self.chunks == 1:
            return device
        chip, core = self.place()
        other = lax.bitwise_xor(lax.rem(device, 2), core)
        return other * self.chunks + lax.bitwise_xor(lax.div(device, 2), chip)

    def device_of(self, slot):
        if self.chunks == 1:
            return slot
        chip, core = self.place()
        return lax.bitwise_xor(chip, slot % self.chunks) * 2 + lax.bitwise_xor(core, slot // self.chunks)

    def target(self, k):
        if self.chunks == 1:
            return lax.axis_index(AXIS)
        chip, core = self.place()
        return lax.bitwise_xor(chip, k) * 2 + core


def split_three(values):
    high = values.astype(bf16)
    rest = values - high.astype(f32)
    middle = rest.astype(bf16)
    low = (rest - middle.astype(f32)).astype(bf16)
    return high.astype(f32), middle.astype(f32), low.astype(f32)


def fold_rows(values):
    return values.reshape(-1, 8, values.shape[-1]).sum(axis=0)


def column_sums(values_of, rows, valid):
    pixels = jnp.int32(0)
    total = None
    for row in rows:
        values = values_of(row)
        inside = row < valid
        pixels = pixels + jnp.where(inside, values.shape[0], 0)
        part = jnp.where(inside, fold_rows(values), 0.0)
        total = part if total is None else total + part
    total = jnp.sum(total, axis=0, keepdims=True)
    mean = total / jnp.maximum(pixels, 1).astype(f32)
    spread = None
    for row in rows:
        apart = values_of(row) - mean
        part = jnp.where(row < valid, fold_rows(apart * apart), 0.0)
        spread = part if spread is None else spread + part
    return pixels.astype(f32), total, jnp.sum(spread, axis=0, keepdims=True)


def pack_stats(plan, sums, spreads):
    parts = list(split_three(jnp.concatenate(sums + spreads, axis=0)))
    padding = plan.stat_rows - 6 * plan.count
    if padding:
        parts.append(jnp.zeros((padding, plan.channels), f32))
    return jnp.concatenate(parts, axis=0).astype(bf16)


def fill_buffers(plan, stats, edge_of, columns, buf_refs):
    for k in range(plan.chunks):
        buf_refs[k][0 : plan.stat_rows, :] = stats
        start = plan.chunk(k) * plan.width
        if plan.chunks > 1:
            start = pl.multiple_of(start, 16)
        for tile in range(plan.count):
            for edge in range(2):
                at = plan.row_base + (2 * tile + edge) * plan.width
                buf_refs[k][at : at + plan.width, :] = edge_of(tile, edge, pl.ds(start, plan.width))
        for place, column in enumerate(columns):
            at = plan.col_base + place * plan.rows
            buf_refs[k][at : at + plan.rows, :] = column


def own_values(plan, ref):
    first = lax.axis_index(AXIS) * plan.count
    return [ref[first + tile] for tile in range(plan.count)]


def edges_kernel(plan, rows_hbm, x_hbm, *refs):
    buf_refs, (rows_ref, x_ref, sems) = refs[: plan.chunks], refs[plan.chunks :]
    counts = pltpu.make_async_copy(rows_hbm, rows_ref, sems.at[plan.count])
    counts.start()
    copies = [pltpu.make_async_copy(x_hbm.at[tile], x_ref.at[tile], sems.at[tile]) for tile in range(plan.count)]
    for copy in copies:
        copy.start()
    counts.wait()
    own_rows = own_values(plan, rows_ref)
    sums, spreads, columns = [], [], []
    for tile in range(plan.count):
        copies[tile].wait()
        _, total, spread = column_sums(lambda row: x_ref[tile, row].astype(f32), range(plan.rows), own_rows[tile])
        sums.append(total)
        spreads.append(spread)
        for column in (0, plan.cols - 1):
            picked = [x_ref[tile, row, column : column + 1, :].astype(f32) for row in range(plan.rows)]
            columns.append(jnp.concatenate(picked, axis=0).astype(bf16))

    def edge_of(tile, edge, window):
        return x_ref[tile, edge * (plan.rows - 1), window, :]

    fill_buffers(plan, pack_stats(plan, sums, spreads), edge_of, columns, buf_refs)


def group_total(values, group_width):
    lanes = values.shape[-1]
    lane = lax.broadcasted_iota(jnp.int32, values.shape, 1)
    step = 1
    while step < group_width:
        ahead = pltpu.roll(values, lanes - step, axis=1)
        behind = pltpu.roll(values, step, axis=1)
        values = values + jnp.where(lax.bitwise_and(lane, step) == 0, ahead, behind)
        step *= 2
    return values


class Held:
    def __init__(self, plan, bufs, held):
        self.plan = plan
        if plan.chunks > 1:
            for slot in range(plan.slots):
                held[slot] = bufs[slot][...]
            self.held = held
        else:
            self.held = bufs[0]

    def locate(self, tile):
        tile = jnp.maximum(tile, 0)
        return self.plan.slot_of(lax.div(tile, self.plan.count)), lax.rem(tile, self.plan.count)

    def edge_row(self, tile, edge):
        slot, local = self.locate(tile)
        at = pl.multiple_of(self.plan.row_base + (2 * local + edge) * self.plan.width, 16)
        return self.held[slot, pl.ds(at, self.plan.width), :]

    def edge_col(self, tile, edge):
        slot, local = self.locate(tile)
        at = pl.multiple_of(self.plan.col_base + (2 * local + edge) * self.plan.rows, 16)
        return self.held[slot, pl.ds(at, self.plan.rows), :]


def buffer_inputs(plan, refs):
    inputs = plan.slots if plan.chunks > 1 else 1
    return refs[:inputs], refs[inputs:]


def route_kernel(plan, links_ref, *refs):
    bufs, refs = buffer_inputs(plan, refs)
    send_refs, held = refs[:-1], Held(plan, bufs, refs[-1])
    for k in range(plan.chunks):
        first = plan.target(k) * plan.count
        for tile in range(plan.count):
            for edge in range(2):
                at = (2 * tile + edge) * plan.width
                wanted = links_ref[(first + tile) * 4 + edge]
                send_refs[k][at : at + plan.width, :] = held.edge_row(wanted, 1 - edge)


def image_norms(plan, rows_ref, image_ref, held):
    count, channels = plan.count, plan.channels
    group_width = channels // G
    first = lax.axis_index(AXIS) * count
    partial = []
    for slot in range(plan.slots):
        raw = held[slot, 0 : plan.stat_rows, :].astype(f32)
        span = 2 * count
        partial.append(raw[0:span] + raw[span : 2 * span] + raw[2 * span : 3 * span])
    means, inverses = [], []
    for tile in range(count):
        image = image_ref[first + tile]
        weights, pixels = [], []
        area = jnp.int32(0)
        for slot in range(plan.slots):
            base = plan.device_of(slot) * count
            for other in range(count):
                same = image_ref[base + other] == image
                weights.append(jnp.where(same, 1.0, 0.0).astype(f32))
                amount = rows_ref[base + other] * plan.cols
                pixels.append(jnp.maximum(amount, 1).astype(f32))
                area = area + jnp.where(same, amount, 0)
        total = jnp.zeros((1, channels), f32)
        for slot in range(plan.slots):
            for other in range(count):
                total = total + weights[slot * count + other] * partial[slot][other : other + 1]
        amount = jnp.maximum(area * group_width, 1).astype(f32)
        mean = group_total(jnp.broadcast_to(total, (8, channels)), group_width)[0:1] / amount
        total = jnp.zeros((1, channels), f32)
        for slot in range(plan.slots):
            for other in range(count):
                place = slot * count + other
                apart = partial[slot][other : other + 1] / pixels[place] - mean
                spread = partial[slot][count + other : count + other + 1] + pixels[place] * apart * apart
                total = total + weights[place] * spread
        variance = group_total(jnp.broadcast_to(total, (8, channels)), group_width)[0:1] / amount
        means.append(mean)
        inverses.append(lax.rsqrt(variance + epsilon))
    return means, inverses


def halves(mean, inverse, gain_ref, shift_ref):
    scale = inverse * (gain_ref[...] * 0.5)
    shift = shift_ref[...] * 0.5

    def activate(values):
        half = (values.astype(f32) - mean) * scale + shift
        return half + half * jnp.tanh(half)

    return activate


def taps(act, before, after):
    cols = act.shape[0]
    pixel = lax.broadcasted_iota(jnp.int32, act.shape, 0)
    back = jnp.where(pixel == 0, before, pltpu.roll(act, 1, axis=0))
    ahead = jnp.where(pixel == cols - 1, after, pltpu.roll(act, cols - 1, axis=0))
    return [values.astype(bf16) for values in (back, act, ahead)]


def middle_kernel(plan, last, links_ref, rows_ref, image_ref, *refs):
    bufs, refs = buffer_inputs(plan, refs)
    x_ref, gain_ref, shift_ref, offset_ref, weight_ref = refs[:5]
    refs = refs[5:]
    ends_ref = residual_ref = None
    if last:
        (ends_ref, residual_ref), refs = refs[:2], refs[2:]
    out_ref, partial_ref, norm_ref, side_ref, held_ref, wide = refs[:6]
    refs = refs[6:]
    count, rows, cols, channels = plan.count, plan.rows, plan.cols, plan.channels
    held = Held(plan, bufs, held_ref)
    means, inverses = image_norms(plan, rows_ref, image_ref, held.held)
    first = lax.axis_index(AXIS) * count
    own_rows = own_values(plan, rows_ref)
    offset = offset_ref[...]
    norm_ref[0 : 2 * count, :] = jnp.concatenate(means + inverses, axis=0)
    copies = []
    for tile in range(count):
        valid = own_rows[tile]
        link = [links_ref[(first + tile) * 4 + column] for column in range(4)]
        activate = halves(means[tile], inverses[tile], gain_ref, shift_ref)
        left = jnp.where(link[2] >= 0, activate(held.edge_col(link[2], 1)), 0.0)
        right = jnp.where(link[3] >= 0, activate(held.edge_col(link[3], 0)), 0.0)
        corners = []
        for place in range(4):
            beside = links_ref[jnp.maximum(link[place // 2], 0) * 4 + 2 + place % 2]
            beside = jnp.where(link[place // 2] >= 0, beside, -1)
            row = 0 if place // 2 else rows - 1
            corner = activate(held.edge_col(beside, 1 - place % 2))[row : row + 1]
            corners.append(jnp.where(beside >= 0, corner, 0.0))
        side_ref[8 * tile : 8 * tile + 4, :] = jnp.concatenate(corners, axis=0)

        depth = 3 * channels
        nothing = jnp.zeros((cols, depth), bf16)
        wide[tile, 0, :, 0:depth] = nothing
        wide[tile, rows // 2, :, depth : 2 * depth] = nothing
        for row in range(rows):
            if ends_ref is not None and row in (0, rows - 1):
                source = ends_ref[2 * tile + (row > 0)]
            else:
                source = x_ref[tile, row]
            act = jnp.where(row < valid, activate(source), 0.0)
            before = jnp.where(row < valid, left[row : row + 1], 0.0)
            after = jnp.where(row < valid, right[row : row + 1], 0.0)
            lane = ((row + 1) % 2) * depth
            for tap, values in enumerate(taps(act, before, after)):
                at = lane + tap * channels
                wide[tile, (row + 1) // 2, :, at : at + channels] = values

        pairs = rows // 2
        upper = wide[tile, 0:pairs].reshape(pairs * cols, 2 * depth)
        lower = wide[tile, 1 : pairs + 1].reshape(pairs * cols, 2 * depth)
        summed = jnp.dot(upper, weight_ref[0 : 2 * depth, :], preferred_element_type=f32)
        summed = summed + jnp.dot(lower, weight_ref[2 * depth : 4 * depth, :], preferred_element_type=f32)
        for row in range(rows):
            at, lane = (row // 2) * cols, (row % 2) * channels
            part = summed[at : at + cols, lane : lane + channels] + offset
            if last:
                part = part + residual_ref[tile, row].astype(f32)
            if row in (0, rows - 1):
                partial_ref[2 * tile + (row > 0)] = part
            elif last:
                refs[0][tile, row] = jnp.where(row < valid, part, 0.0).astype(bf16)
            else:
                out_ref[tile, row] = jnp.where(row < valid, part, 0.0).astype(bf16)
        if last:
            window = pl.ds(1, rows - 2)
            copy = pltpu.make_async_copy(refs[0].at[tile, window], out_ref.at[tile, window], refs[1].at[tile])
            copy.start()
            copies.append(copy)
        else:
            _, total, spread = column_sums(
                lambda row: out_ref[tile, row].astype(f32), range(1, rows - 1), valid
            )
            norm_ref[(2 * count + tile) : (2 * count + tile) + 1, :] = total
            norm_ref[(3 * count + tile) : (3 * count + tile) + 1, :] = spread
            for side, column in enumerate((0, cols - 1)):
                picked = [out_ref[tile, row, column : column + 1, :].astype(f32) for row in range(1, rows - 1)]
                at = 8 * count + (2 * tile + side) * rows
                side_ref[at + 1 : at + rows - 1, :] = jnp.concatenate(picked, axis=0)
    for copy in copies:
        copy.wait()


def ends_kernel(plan, last, links_ref, rows_ref, *refs):
    halo_refs, refs = refs[: plan.chunks], refs[plan.chunks :]
    partial_ref, norm_ref, side_ref, gain_ref, shift_ref, weight_ref = refs[:6]
    refs = refs[6:]
    count, rows, cols, channels = plan.count, plan.rows, plan.cols, plan.channels
    if last:
        _, out_ref, halo, ends_ref, sems = refs
    else:
        ends_ref, buf_refs, halo = refs[0], refs[1:-1], refs[-1]
    first = lax.axis_index(AXIS) * count
    own_rows = own_values(plan, rows_ref)
    for k in range(plan.chunks):
        start = plan.chunk(k) * plan.width
        if plan.chunks > 1:
            start = pl.multiple_of(start, 16)
        for place in range(2 * count):
            at = place * plan.width
            halo[place, pl.ds(start, plan.width), :] = halo_refs[k][at : at + plan.width, :]
    depth = 3 * channels
    copies, sums, spreads, columns = [], [], [], []
    for tile in range(count):
        valid = own_rows[tile]
        activate = halves(
            norm_ref[tile : tile + 1, :], norm_ref[count + tile : count + tile + 1, :], gain_ref, shift_ref
        )
        values = []
        for edge, row in enumerate((0, rows - 1)):
            place = 2 * tile + edge
            present = links_ref[(first + tile) * 4 + edge] >= 0
            act = jnp.where(present, activate(halo[place]), 0.0)
            at = 8 * tile + 2 * edge
            wide = jnp.concatenate(taps(act, side_ref[at : at + 1, :], side_ref[at + 1 : at + 2, :]), axis=1)
            weight = weight_ref[3 * edge * depth : (3 * edge + 1) * depth, edge * channels : (edge + 1) * channels]
            part = partial_ref[place] + jnp.dot(wide, weight, preferred_element_type=f32)
            result = jnp.where(row < valid, part, 0.0).astype(bf16)
            ends_ref[place] = result
            values.append(result.astype(f32))
            if last:
                copies.append(pltpu.make_async_copy(ends_ref.at[place], out_ref.at[tile, row], sems.at[place]))
                copies[-1].start()
        if last:
            continue
        amount, total, spread = column_sums(lambda row: values[row > 0], (0, rows - 1), valid)
        inner_total = norm_ref[2 * count + tile : 2 * count + tile + 1, :]
        inner_spread = norm_ref[3 * count + tile : 3 * count + tile + 1, :]
        inner = jnp.maximum((jnp.minimum(valid, rows - 1) - 1) * cols, 1).astype(f32)
        amount = jnp.maximum(amount, 1.0)
        apart = inner_total / inner - total / amount
        sums.append(inner_total + total)
        spreads.append(inner_spread + spread + apart * apart * (inner * amount / (inner + amount)))
        line = lax.broadcasted_iota(jnp.int32, (rows, channels), 0)
        for side, column in enumerate((0, cols - 1)):
            at = 8 * count + (2 * tile + side) * rows
            picked = side_ref[at : at + rows, :]
            picked = jnp.where(line == 0, values[0][column : column + 1], picked)
            picked = jnp.where(line == rows - 1, values[1][column : column + 1], picked)
            columns.append(picked.astype(bf16))
    if not last:

        def edge_of(tile, edge, window):
            return ends_ref[2 * tile + edge, window, :]

        fill_buffers(plan, pack_stats(plan, sums, spreads), edge_of, columns, buf_refs)
    for copy in copies:
        copy.wait()


def paired_weights(kernel):
    upper = jnp.pad(kernel, ((0, 1), (0, 0), (0, 0), (0, 0)))
    lower = jnp.pad(kernel, ((1, 0), (0, 0), (0, 0), (0, 0)))
    both = jnp.concatenate([upper, lower], axis=-1)
    return both.reshape(-1, both.shape[-1])


def shards(
    feature_tiles,
    neighbours,
    valid_rows,
    tile_image,
    gain_one,
    shift_one,
    kernel_one,
    offset_one,
    gain_two,
    shift_two,
    kernel_two,
    offset_two,
    *,
    size,
):
    count, rows, cols, channels = feature_tiles.shape
    plan = Plan(size, count, rows, cols, channels)
    links = neighbours.reshape(-1)
    scalars = (links, valid_rows, tile_image)
    buf_shape = [jax.ShapeDtypeStruct((plan.buf_rows, channels), bf16)] * plan.chunks
    limit = 24 * 1024 * 1024
    params = pltpu.CompilerParams(vmem_limit_bytes=limit)

    def swap(array, distance):
        return lax.ppermute(array, AXIS, [(i, i ^ distance) for i in range(size)])

    def spread(arrays):
        result = [arrays[0]]
        for k in range(1, plan.chunks):
            result.append(swap(arrays[k], 2 * k))
        return result

    def exchange(bufs):
        if plan.chunks == 1:
            return [lax.all_gather(bufs[0], AXIS)]
        own = spread(bufs)
        return own + [swap(array, 1) for array in own]

    def shape(dims, dtype=f32):
        return jax.ShapeDtypeStruct(dims, dtype)

    held = pltpu.VMEM((plan.slots, plan.buf_rows, channels) if plan.chunks > 1 else (1, 16, channels), bf16)
    partial_shape = shape((2 * count, cols, channels))
    norm_shape = shape((round_up(4 * count, 8), channels))
    side_shape = shape((8 * count + 2 * count * rows, channels))
    ends_shape = shape((2 * count, cols, channels), bf16)
    tiles_shape = shape(feature_tiles.shape, bf16)

    def stage(last, source, ends, bufs, gain, shift, kernel, offset):
        arrays = exchange(bufs)
        send = pl.pallas_call(
            functools.partial(route_kernel, plan),
            out_shape=[shape((2 * count * plan.width, channels), bf16)] * plan.chunks,
            in_specs=[SMEM] + [VMEM] * len(arrays),
            out_specs=[VMEM] * plan.chunks,
            scratch_shapes=[held],
            compiler_params=params,
        )(links, *arrays)
        halo = spread(send)
        weights = paired_weights(kernel)
        gain, shift, offset = gain[None], shift[None], offset[None]
        operands = arrays + [source, gain, shift, offset, weights] + ([ends, feature_tiles] if last else [])
        flops = 2 * count * rows * cols * 9 * channels * channels
        tiles, partial, norm, side = pl.pallas_call(
            functools.partial(middle_kernel, plan, last),
            out_shape=[tiles_shape, partial_shape, norm_shape, side_shape],
            in_specs=[SMEM] * 3 + [VMEM] * len(operands),
            out_specs=[HBM if last else VMEM] + [VMEM] * 3,
            scratch_shapes=[held, pltpu.VMEM((count, rows // 2 + 1, cols, 6 * channels), bf16)]
            + ([pltpu.VMEM(feature_tiles.shape, bf16), pltpu.SemaphoreType.DMA((count,))] if last else []),
            compiler_params=params,
            cost_estimate=pl.CostEstimate(flops=flops, bytes_accessed=4 * feature_tiles.size, transcendentals=0),
        )(*scalars, *operands)
        operands = halo + [partial, norm, side, gain, shift, weights]
        scratch = [pltpu.VMEM((2 * count, cols, channels), bf16)]
        if last:
            return pl.pallas_call(
                functools.partial(ends_kernel, plan, last),
                out_shape=tiles_shape,
                in_specs=[SMEM] * 2 + [VMEM] * len(operands) + [HBM],
                out_specs=HBM,
                input_output_aliases={2 + len(operands): 0},
                scratch_shapes=scratch + scratch + [pltpu.SemaphoreType.DMA((2 * count,))],
                compiler_params=params,
            )(links, valid_rows, *operands, tiles)
        ends, *bufs = pl.pallas_call(
            functools.partial(ends_kernel, plan, last),
            out_shape=[ends_shape] + buf_shape,
            in_specs=[SMEM] * 2 + [VMEM] * len(operands),
            out_specs=[VMEM] * (1 + plan.chunks),
            scratch_shapes=scratch,
            compiler_params=params,
        )(links, valid_rows, *operands)
        return tiles, ends, bufs

    bufs = pl.pallas_call(
        functools.partial(edges_kernel, plan),
        out_shape=buf_shape,
        in_specs=[HBM, HBM],
        out_specs=[VMEM] * plan.chunks,
        scratch_shapes=[
            pltpu.SMEM(valid_rows.shape, jnp.int32),
            pltpu.VMEM(feature_tiles.shape, bf16),
            pltpu.SemaphoreType.DMA((count + 1,)),
        ],
        compiler_params=params,
        name="edges",
    )(valid_rows, feature_tiles)
    hidden, ends, bufs = stage(False, feature_tiles, None, bufs, gain_one, shift_one, kernel_one, offset_one)
    return stage(True, hidden, ends, bufs, gain_two, shift_two, kernel_two, offset_two)


def solution(mesh):
    in_specs = (
        P(("rep", "tile"), None, None, None),
        P("rep", None),
        P("rep"),
        P("rep"),
        P(),
        P(),
        P(),
        P(),
        P(),
        P(),
        P(),
        P(),
    )
    out_specs = P(("rep", "tile"), None, None, None)

    def body(*args):
        return shards(*args, size=mesh.shape[AXIS])

    return jax.shard_map(body, mesh=mesh, in_specs=in_specs, out_specs=out_specs, check_vma=False)
```

```python
import functools

import jax
import jax.numpy as jnp
from jax import lax
from jax.experimental import pallas as pl
from jax.experimental.pallas import tpu as pltpu
from jax.sharding import PartitionSpec as P


G = 32
AXIS = "tile"
epsilon = 1e-06
f32 = jnp.float32
bf16 = jnp.bfloat16


VMEM = pl.BlockSpec(memory_space=pltpu.VMEM)
SMEM = pl.BlockSpec(memory_space=pltpu.SMEM)
HBM = pl.BlockSpec(memory_space=pltpu.HBM)


def round_up(value, step):
    return -(-value // step) * step


class Plan:
    def __init__(self, size, count, rows, cols, channels):
        self.size, self.count, self.rows, self.cols, self.channels = size, count, rows, cols, channels
        chips = size // 2
        fits = size % 2 == 0 and chips & (chips - 1) == 0 and cols % (16 * max(chips, 1)) == 0
        self.chunks = chips if fits and chips > 1 else 1
        self.width = cols // self.chunks
        self.stat_rows = round_up(6 * count, 16)
        self.row_base = self.stat_rows
        self.col_base = self.row_base + 2 * count * self.width
        self.buf_rows = self.col_base + 2 * count * rows
        self.slots = size

    def place(self):
        index = lax.axis_index(AXIS)
        return lax.div(index, 2), lax.rem(index, 2)

    def chunk(self, k):
        return lax.bitwise_xor(self.place()[0], k) if self.chunks > 1 else 0

    def slot_of(self, device):
        if self.chunks == 1:
            return device
        chip, core = self.place()
        other = lax.bitwise_xor(lax.rem(device, 2), core)
        return other * self.chunks + lax.bitwise_xor(lax.div(device, 2), chip)

    def device_of(self, slot):
        if self.chunks == 1:
            return slot
        chip, core = self.place()
        return lax.bitwise_xor(chip, slot % self.chunks) * 2 + lax.bitwise_xor(core, slot // self.chunks)

    def target(self, k):
        if self.chunks == 1:
            return lax.axis_index(AXIS)
        chip, core = self.place()
        return lax.bitwise_xor(chip, k) * 2 + core


def split_three(values):
    high = values.astype(bf16)
    rest = values - high.astype(f32)
    middle = rest.astype(bf16)
    low = (rest - middle.astype(f32)).astype(bf16)
    return high.astype(f32), middle.astype(f32), low.astype(f32)


def fold_rows(values):
    return values.reshape(-1, 8, values.shape[-1]).sum(axis=0)


def column_sums(values_of, rows, valid):
    pixels = jnp.int32(0)
    total = None
    for row in rows:
        values = values_of(row)
        inside = row < valid
        pixels = pixels + jnp.where(inside, values.shape[0], 0)
        part = jnp.where(inside, fold_rows(values), 0.0)
        total = part if total is None else total + part
    total = jnp.sum(total, axis=0, keepdims=True)
    mean = total / jnp.maximum(pixels, 1).astype(f32)
    spread = None
    for row in rows:
        apart = values_of(row) - mean
        part = jnp.where(row < valid, fold_rows(apart * apart), 0.0)
        spread = part if spread is None else spread + part
    return pixels.astype(f32), total, jnp.sum(spread, axis=0, keepdims=True)


def merge_sums(one, two):
    pixels, other = jnp.maximum(one[0], 1.0), jnp.maximum(two[0], 1.0)
    apart = one[1] / pixels - two[1] / other
    weight = jnp.where(jnp.minimum(one[0], two[0]) > 0, pixels * other / (pixels + other), 0.0)
    return one[0] + two[0], one[1] + two[1], one[2] + two[2] + apart * apart * weight


def pack_stats(plan, sums, spreads):
    parts = list(split_three(jnp.concatenate(sums + spreads, axis=0)))
    padding = plan.stat_rows - 6 * plan.count
    if padding:
        parts.append(jnp.zeros((padding, plan.channels), f32))
    return jnp.concatenate(parts, axis=0).astype(bf16)


def fill_buffers(plan, stats, edge_of, columns, buf_refs):
    for k in range(plan.chunks):
        buf_refs[k][0 : plan.stat_rows, :] = stats
        start = plan.chunk(k) * plan.width
        if plan.chunks > 1:
            start = pl.multiple_of(start, 16)
        for tile in range(plan.count):
            for edge in range(2):
                at = plan.row_base + (2 * tile + edge) * plan.width
                buf_refs[k][at : at + plan.width, :] = edge_of(tile, edge, pl.ds(start, plan.width))
        for place, column in enumerate(columns):
            at = plan.col_base + place * plan.rows
            buf_refs[k][at : at + plan.rows, :] = column


def own_values(plan, ref):
    first = lax.axis_index(AXIS) * plan.count
    return [ref[first + tile] for tile in range(plan.count)]


def edges_kernel(plan, links_hbm, rows_hbm, image_hbm, x_hbm, links_ref, rows_ref, image_ref, *refs):
    buf_refs, (x_ref, sems) = refs[: plan.chunks], refs[plan.chunks :]
    tables = [
        pltpu.make_async_copy(source, target, sems.at[plan.count + place])
        for place, (source, target) in enumerate(
            ((rows_hbm, rows_ref), (links_hbm, links_ref), (image_hbm, image_ref))
        )
    ]
    copies = [pltpu.make_async_copy(x_hbm.at[tile], x_ref.at[tile], sems.at[tile]) for tile in range(plan.count)]
    for copy in tables[:1] + copies + tables[1:]:
        copy.start()
    for copy in tables:
        copy.wait()
    own_rows = own_values(plan, rows_ref)
    sums, spreads, columns = [], [], []
    for tile in range(plan.count):
        copies[tile].wait()
        _, total, spread = column_sums(lambda row: x_ref[tile, row].astype(f32), range(plan.rows), own_rows[tile])
        sums.append(total)
        spreads.append(spread)
        for column in (0, plan.cols - 1):
            picked = [x_ref[tile, row, column : column + 1, :].astype(f32) for row in range(plan.rows)]
            columns.append(jnp.concatenate(picked, axis=0).astype(bf16))

    def edge_of(tile, edge, window):
        return x_ref[tile, edge * (plan.rows - 1), window, :]

    fill_buffers(plan, pack_stats(plan, sums, spreads), edge_of, columns, buf_refs)


def group_total(values, group_width):
    lanes = values.shape[-1]
    lane = lax.broadcasted_iota(jnp.int32, values.shape, 1)
    step = 1
    while step < group_width:
        ahead = pltpu.roll(values, lanes - step, axis=1)
        behind = pltpu.roll(values, step, axis=1)
        values = values + jnp.where(lax.bitwise_and(lane, step) == 0, ahead, behind)
        step *= 2
    return values


class Held:
    def __init__(self, plan, bufs, held, part):
        self.plan = plan
        self.row_base, self.col_base = plan.row_base, plan.col_base
        self.held = bufs[0]
        if plan.chunks > 1:
            self.held = held
            self.row_base, self.col_base = 0, plan.stat_rows
            for slot in range(plan.slots):
                if part == "rows":
                    held[slot] = bufs[slot][plan.row_base : plan.col_base, :]
                else:
                    held[slot, 0 : plan.stat_rows, :] = bufs[slot][0 : plan.stat_rows, :]
                    held[slot, plan.stat_rows :, :] = bufs[slot][plan.col_base :, :]

    def locate(self, tile):
        tile = jnp.maximum(tile, 0)
        return self.plan.slot_of(lax.div(tile, self.plan.count)), lax.rem(tile, self.plan.count)

    def edge_row(self, tile, edge):
        slot, local = self.locate(tile)
        at = pl.multiple_of(self.row_base + (2 * local + edge) * self.plan.width, 16)
        return self.held[slot, pl.ds(at, self.plan.width), :]

    def edge_col(self, tile, edge):
        slot, local = self.locate(tile)
        at = pl.multiple_of(self.col_base + (2 * local + edge) * self.plan.rows, 16)
        return self.held[slot, pl.ds(at, self.plan.rows), :]


def held_scratch(plan, part):
    rows = plan.col_base - plan.row_base if part == "rows" else plan.buf_rows - plan.col_base + plan.stat_rows
    return pltpu.VMEM((plan.slots, rows, plan.channels) if plan.chunks > 1 else (1, 16, plan.channels), bf16)


def buffer_inputs(plan, refs):
    inputs = plan.slots if plan.chunks > 1 else 1
    return refs[:inputs], refs[inputs:]


def route_kernel(plan, links_ref, *refs):
    bufs, refs = buffer_inputs(plan, refs)
    send_refs, held = refs[:-1], Held(plan, bufs, refs[-1], "rows")
    for k in range(plan.chunks):
        first = plan.target(k) * plan.count
        for tile in range(plan.count):
            for edge in range(2):
                at = (2 * tile + edge) * plan.width
                wanted = links_ref[edge, first + tile]
                send_refs[k][at : at + plan.width, :] = held.edge_row(wanted, 1 - edge)


def image_norms(plan, rows_ref, image_ref, held):
    count, channels = plan.count, plan.channels
    group_width = channels // G
    first = lax.axis_index(AXIS) * count
    partial = []
    for slot in range(plan.slots):
        raw = held[slot, 0 : plan.stat_rows, :].astype(f32)
        span = 2 * count
        partial.append(raw[0:span] + raw[span : 2 * span] + raw[2 * span : 3 * span])
    means, inverses = [], []
    for tile in range(count):
        image = image_ref[first + tile]
        weights, pixels = [], []
        area = jnp.int32(0)
        for slot in range(plan.slots):
            base = plan.device_of(slot) * count
            for other in range(count):
                same = image_ref[base + other] == image
                weights.append(jnp.where(same, 1.0, 0.0).astype(f32))
                amount = rows_ref[base + other] * plan.cols
                pixels.append(jnp.maximum(amount, 1).astype(f32))
                area = area + jnp.where(same, amount, 0)
        total = jnp.zeros((1, channels), f32)
        for slot in range(plan.slots):
            for other in range(count):
                total = total + weights[slot * count + other] * partial[slot][other : other + 1]
        amount = jnp.maximum(area * group_width, 1).astype(f32)
        mean = group_total(jnp.broadcast_to(total, (8, channels)), group_width)[0:1] / amount
        total = jnp.zeros((1, channels), f32)
        for slot in range(plan.slots):
            for other in range(count):
                place = slot * count + other
                apart = partial[slot][other : other + 1] / pixels[place] - mean
                spread = partial[slot][count + other : count + other + 1] + pixels[place] * apart * apart
                total = total + weights[place] * spread
        variance = group_total(jnp.broadcast_to(total, (8, channels)), group_width)[0:1] / amount
        means.append(mean)
        inverses.append(lax.rsqrt(variance + epsilon))
    return means, inverses


def halves(mean, inverse, gain_ref, shift_ref):
    scale = inverse * (gain_ref[...] * 0.5)
    shift = shift_ref[...] * 0.5

    def activate(values):
        half = (values.astype(f32) - mean) * scale + shift
        return half + half * jnp.tanh(half)

    return activate


def taps(act, before, after):
    cols = act.shape[0]
    pixel = lax.broadcasted_iota(jnp.int32, act.shape, 0)
    back = jnp.where(pixel == 0, before, pltpu.roll(act, 1, axis=0))
    ahead = jnp.where(pixel == cols - 1, after, pltpu.roll(act, cols - 1, axis=0))
    return [values.astype(bf16) for values in (back, act, ahead)]


def middle_kernel(plan, last, links_ref, rows_ref, image_ref, *refs):
    bufs, refs = buffer_inputs(plan, refs)
    x_ref, gain_ref, shift_ref, offset_ref, weight_ref = refs[:5]
    refs = refs[5:]
    ends_ref = residual_ref = None
    if last:
        (ends_ref, residual_ref), refs = refs[:2], refs[2:]
    out_ref, partial_ref, norm_ref, side_ref, held_ref, wide = refs[:6]
    refs = refs[6:]
    count, rows, cols, channels = plan.count, plan.rows, plan.cols, plan.channels
    held = Held(plan, bufs, held_ref, "rest")
    means, inverses = image_norms(plan, rows_ref, image_ref, held.held)
    first = lax.axis_index(AXIS) * count
    own_rows = own_values(plan, rows_ref)
    offset = offset_ref[...]
    norm_ref[0 : 2 * count, :] = jnp.concatenate(means + inverses, axis=0)
    copies = []
    for tile in range(count):
        valid = own_rows[tile]
        link = [links_ref[column, first + tile] for column in range(4)]
        activate = halves(means[tile], inverses[tile], gain_ref, shift_ref)
        left = jnp.where(link[2] >= 0, activate(held.edge_col(link[2], 1)), 0.0)
        right = jnp.where(link[3] >= 0, activate(held.edge_col(link[3], 0)), 0.0)
        corners = []
        for place in range(4):
            beside = links_ref[2 + place % 2, jnp.maximum(link[place // 2], 0)]
            beside = jnp.where(link[place // 2] >= 0, beside, -1)
            row = 0 if place // 2 else rows - 1
            corner = activate(held.edge_col(beside, 1 - place % 2))[row : row + 1]
            corners.append(jnp.where(beside >= 0, corner, 0.0))
        side_ref[8 * tile : 8 * tile + 4, :] = jnp.concatenate(corners, axis=0)

        depth = 3 * channels
        nothing = jnp.zeros((cols, depth), bf16)
        wide[tile, 0, :, 0:depth] = nothing
        wide[tile, rows // 2, :, depth : 2 * depth] = nothing
        for row in range(rows):
            if ends_ref is not None and row in (0, rows - 1):
                source = ends_ref[2 * tile + (row > 0)]
            else:
                source = x_ref[tile, row]
            act = jnp.where(row < valid, activate(source), 0.0)
            before = jnp.where(row < valid, left[row : row + 1], 0.0)
            after = jnp.where(row < valid, right[row : row + 1], 0.0)
            lane = ((row + 1) % 2) * depth
            for tap, values in enumerate(taps(act, before, after)):
                at = lane + tap * channels
                wide[tile, (row + 1) // 2, :, at : at + channels] = values

        pairs = rows // 2
        step = 2 if pairs % 2 == 0 else 1
        gathered = None
        for pair in range(0, pairs, step):
            upper = wide[tile, pair : pair + step].reshape(step * cols, 2 * depth)
            lower = wide[tile, pair + 1 : pair + step + 1].reshape(step * cols, 2 * depth)
            window = jnp.concatenate([upper, lower], axis=1)
            summed = jnp.dot(window, weight_ref[...], preferred_element_type=f32)
            inner = {}
            for row in range(2 * pair, 2 * (pair + step)):
                at, lane = (row // 2 - pair) * cols, (row % 2) * channels
                part = summed[at : at + cols, lane : lane + channels] + offset
                if last:
                    part = part + residual_ref[tile, row].astype(f32)
                if row in (0, rows - 1):
                    partial_ref[2 * tile + (row > 0)] = part
                    continue
                part = jnp.where(row < valid, part, 0.0).astype(bf16)
                if last:
                    refs[0][tile, row] = part
                else:
                    out_ref[tile, row] = part
                inner[row] = part.astype(f32)
            if last:
                band = pl.ds(min(inner), len(inner))
                sem = refs[1].at[tile * pairs + pair]
                copy = pltpu.make_async_copy(refs[0].at[tile, band], out_ref.at[tile, band], sem)
                copy.start()
                copies.append(copy)
            else:
                found = column_sums(lambda row: inner[row], sorted(inner), valid)
                gathered = found if gathered is None else merge_sums(gathered, found)
        if not last:
            norm_ref[(2 * count + tile) : (2 * count + tile) + 1, :] = gathered[1]
            norm_ref[(3 * count + tile) : (3 * count + tile) + 1, :] = gathered[2]
            for side, column in enumerate((0, cols - 1)):
                picked = [out_ref[tile, row, column : column + 1, :].astype(f32) for row in range(1, rows - 1)]
                at = 8 * count + (2 * tile + side) * rows
                side_ref[at + 1 : at + rows - 1, :] = jnp.concatenate(picked, axis=0)
    for copy in copies:
        copy.wait()


def ends_kernel(plan, last, links_ref, rows_ref, *refs):
    halo_refs, refs = refs[: plan.chunks], refs[plan.chunks :]
    partial_ref, norm_ref, side_ref, gain_ref, shift_ref, weight_ref = refs[:6]
    refs = refs[6:]
    count, rows, cols, channels = plan.count, plan.rows, plan.cols, plan.channels
    if last:
        _, out_ref, halo, ends_ref, sems = refs
    else:
        ends_ref, buf_refs, halo = refs[0], refs[1:-1], refs[-1]
    first = lax.axis_index(AXIS) * count
    own_rows = own_values(plan, rows_ref)
    for k in range(plan.chunks):
        start = plan.chunk(k) * plan.width
        if plan.chunks > 1:
            start = pl.multiple_of(start, 16)
        for place in range(2 * count):
            at = place * plan.width
            halo[place, pl.ds(start, plan.width), :] = halo_refs[k][at : at + plan.width, :]
    depth = 3 * channels
    copies, sums, spreads, columns = [], [], [], []
    for tile in range(count):
        valid = own_rows[tile]
        activate = halves(
            norm_ref[tile : tile + 1, :], norm_ref[count + tile : count + tile + 1, :], gain_ref, shift_ref
        )
        values = []
        for edge, row in enumerate((0, rows - 1)):
            place = 2 * tile + edge
            present = links_ref[edge, first + tile] >= 0
            act = jnp.where(present, activate(halo[place]), 0.0)
            at = 8 * tile + 2 * edge
            wide = jnp.concatenate(taps(act, side_ref[at : at + 1, :], side_ref[at + 1 : at + 2, :]), axis=1)
            weight = weight_ref[3 * edge * depth : (3 * edge + 1) * depth, edge * channels : (edge + 1) * channels]
            part = partial_ref[place] + jnp.dot(wide, weight, preferred_element_type=f32)
            result = jnp.where(row < valid, part, 0.0).astype(bf16)
            ends_ref[place] = result
            values.append(result.astype(f32))
            if last:
                copies.append(pltpu.make_async_copy(ends_ref.at[place], out_ref.at[tile, row], sems.at[place]))
                copies[-1].start()
        if last:
            continue
        found = column_sums(lambda row: values[row > 0], (0, rows - 1), valid)
        inner = (
            jnp.maximum((jnp.minimum(valid, rows - 1) - 1) * cols, 0).astype(f32),
            norm_ref[2 * count + tile : 2 * count + tile + 1, :],
            norm_ref[3 * count + tile : 3 * count + tile + 1, :],
        )
        _, total, spread = merge_sums(inner, found)
        sums.append(total)
        spreads.append(spread)
        line = lax.broadcasted_iota(jnp.int32, (rows, channels), 0)
        for side, column in enumerate((0, cols - 1)):
            at = 8 * count + (2 * tile + side) * rows
            picked = side_ref[at : at + rows, :]
            picked = jnp.where(line == 0, values[0][column : column + 1], picked)
            picked = jnp.where(line == rows - 1, values[1][column : column + 1], picked)
            columns.append(picked.astype(bf16))
    if not last:

        def edge_of(tile, edge, window):
            return ends_ref[2 * tile + edge, window, :]

        fill_buffers(plan, pack_stats(plan, sums, spreads), edge_of, columns, buf_refs)
    for copy in copies:
        copy.wait()


def paired_weights(kernel):
    upper = jnp.pad(kernel, ((0, 1), (0, 0), (0, 0), (0, 0)))
    lower = jnp.pad(kernel, ((1, 0), (0, 0), (0, 0), (0, 0)))
    both = jnp.concatenate([upper, lower], axis=-1)
    return both.reshape(-1, both.shape[-1])


def shards(
    feature_tiles,
    neighbours,
    valid_rows,
    tile_image,
    gain_one,
    shift_one,
    kernel_one,
    offset_one,
    gain_two,
    shift_two,
    kernel_two,
    offset_two,
    *,
    size,
):
    count, rows, cols, channels = feature_tiles.shape
    plan = Plan(size, count, rows, cols, channels)
    buf_shape = [jax.ShapeDtypeStruct((plan.buf_rows, channels), bf16)] * plan.chunks
    limit = 24 * 1024 * 1024
    params = pltpu.CompilerParams(vmem_limit_bytes=limit)

    def swap(array, distance):
        return lax.ppermute(array, AXIS, [(i, i ^ distance) for i in range(size)])

    def spread(arrays):
        result = [arrays[0]]
        for k in range(1, plan.chunks):
            result.append(swap(arrays[k], 2 * k))
        return result

    def exchange(bufs):
        if plan.chunks == 1:
            return [lax.all_gather(bufs[0], AXIS)]
        own = spread(bufs)
        return own + [swap(array, 1) for array in own]

    def shape(dims, dtype=f32):
        return jax.ShapeDtypeStruct(dims, dtype)

    partial_shape = shape((2 * count, cols, channels))
    norm_shape = shape((round_up(4 * count, 8), channels))
    side_shape = shape((8 * count + 2 * count * rows, channels))
    ends_shape = shape((2 * count, cols, channels), bf16)
    tiles_shape = shape(feature_tiles.shape, bf16)

    def stage(last, source, ends, bufs, gain, shift, kernel, offset):
        arrays = exchange(bufs)
        send = pl.pallas_call(
            functools.partial(route_kernel, plan),
            out_shape=[shape((2 * count * plan.width, channels), bf16)] * plan.chunks,
            in_specs=[SMEM] + [VMEM] * len(arrays),
            out_specs=[VMEM] * plan.chunks,
            scratch_shapes=[held_scratch(plan, "rows")],
            compiler_params=params,
        )(scalars[0], *arrays)
        halo = spread(send)
        weights = paired_weights(kernel)
        gain, shift, offset = gain[None], shift[None], offset[None]
        operands = arrays + [source, gain, shift, offset, weights] + ([ends, feature_tiles] if last else [])
        flops = 2 * count * rows * cols * 9 * channels * channels
        tiles, partial, norm, side = pl.pallas_call(
            functools.partial(middle_kernel, plan, last),
            out_shape=[tiles_shape, partial_shape, norm_shape, side_shape],
            in_specs=[SMEM] * 3 + [VMEM] * len(operands),
            out_specs=[HBM if last else VMEM] + [VMEM] * 3,
            scratch_shapes=[held_scratch(plan, "rest"), pltpu.VMEM((count, rows // 2 + 1, cols, 6 * channels), bf16)]
            + ([pltpu.VMEM(feature_tiles.shape, bf16), pltpu.SemaphoreType.DMA((count * rows // 2,))] if last else []),
            compiler_params=params,
            cost_estimate=pl.CostEstimate(flops=flops, bytes_accessed=4 * feature_tiles.size, transcendentals=0),
        )(*scalars, *operands)
        operands = halo + [partial, norm, side, gain, shift, weights]
        scratch = [pltpu.VMEM((2 * count, cols, channels), bf16)]
        if last:
            return pl.pallas_call(
                functools.partial(ends_kernel, plan, last),
                out_shape=tiles_shape,
                in_specs=[SMEM] * 2 + [VMEM] * len(operands) + [HBM],
                out_specs=HBM,
                input_output_aliases={2 + len(operands): 0},
                scratch_shapes=scratch + scratch + [pltpu.SemaphoreType.DMA((2 * count,))],
                compiler_params=params,
            )(*scalars[:2], *operands, tiles)
        ends, *bufs = pl.pallas_call(
            functools.partial(ends_kernel, plan, last),
            out_shape=[ends_shape] + buf_shape,
            in_specs=[SMEM] * 2 + [VMEM] * len(operands),
            out_specs=[VMEM] * (1 + plan.chunks),
            scratch_shapes=scratch,
            compiler_params=params,
        )(*scalars[:2], *operands)
        return tiles, ends, bufs

    tables = (neighbours.T, valid_rows, tile_image)
    inputs = [pltpu.with_memory_space_constraint(array, pltpu.HBM) for array in (*tables, feature_tiles)]
    found = pl.pallas_call(
        functools.partial(edges_kernel, plan),
        out_shape=[pltpu.SMEM(table.shape, jnp.int32) for table in tables] + buf_shape,
        in_specs=[HBM] * 4,
        out_specs=[SMEM] * 3 + [VMEM] * plan.chunks,
        scratch_shapes=[pltpu.VMEM(feature_tiles.shape, bf16), pltpu.SemaphoreType.DMA((count + 3,))],
        compiler_params=params,
        name="edges",
    )(*inputs)
    scalars, bufs = found[:3], found[3:]
    hidden, ends, bufs = stage(False, feature_tiles, None, bufs, gain_one, shift_one, kernel_one, offset_one)
    return stage(True, hidden, ends, bufs, gain_two, shift_two, kernel_two, offset_two)


def solution(mesh):
    in_specs = (
        P(("rep", "tile"), None, None, None),
        P("rep", None),
        P("rep"),
        P("rep"),
        P(),
        P(),
        P(),
        P(),
        P(),
        P(),
        P(),
        P(),
    )
    out_specs = P(("rep", "tile"), None, None, None)

    def body(*args):
        return shards(*args, size=mesh.shape[AXIS])

    return jax.shard_map(body, mesh=mesh, in_specs=in_specs, out_specs=out_specs, check_vma=False)
```

```python
import functools

import jax
import jax.numpy as jnp
from jax import lax
from jax.experimental import pallas as pl
from jax.experimental.pallas import tpu as pltpu
from jax.sharding import PartitionSpec as P


G = 32
AXIS = "tile"
epsilon = 1e-06
f32 = jnp.float32
bf16 = jnp.bfloat16


VMEM = pl.BlockSpec(memory_space=pltpu.VMEM)
SMEM = pl.BlockSpec(memory_space=pltpu.SMEM)
HBM = pl.BlockSpec(memory_space=pltpu.HBM)


def round_up(value, step):
    return -(-value // step) * step


class Plan:
    def __init__(self, size, count, rows, cols, channels):
        self.size, self.count, self.rows, self.cols, self.channels = size, count, rows, cols, channels
        chips = size // 2
        self.direct = size % 2 == 0 and chips in (2, 4, 8) and cols % 32 == 0
        self.targets = chips if self.direct else 1
        self.parts = 2 if self.direct else 1
        self.width = cols // self.parts
        self.stat_rows = round_up(6 * count, 16)
        self.row_base = self.stat_rows
        self.col_base = self.row_base + 2 * count * self.width
        self.buf_rows = self.col_base + 2 * count * rows
        self.slots = size

    def place(self):
        index = lax.axis_index(AXIS)
        return lax.div(index, 2), lax.rem(index, 2)

    def window(self, k):
        if not self.direct:
            return pl.ds(0, self.width)
        part = lax.bitwise_and(lax.bitwise_xor(self.place()[0], k), 1)
        return pl.ds(pl.multiple_of(part * self.width, 16), self.width)

    def slot_of(self, device):
        if not self.direct:
            return device
        chip, core = self.place()
        other = lax.bitwise_xor(lax.rem(device, 2), core)
        return other * self.targets + lax.bitwise_xor(lax.div(device, 2), chip)

    def device_of(self, slot):
        if not self.direct:
            return slot
        chip, core = self.place()
        return lax.bitwise_xor(chip, slot % self.targets) * 2 + lax.bitwise_xor(core, slot // self.targets)

    def target(self, k):
        if not self.direct:
            return lax.axis_index(AXIS)
        chip, core = self.place()
        return lax.bitwise_xor(chip, k) * 2 + core


def split_three(values):
    high = values.astype(bf16)
    rest = values - high.astype(f32)
    middle = rest.astype(bf16)
    low = (rest - middle.astype(f32)).astype(bf16)
    return high.astype(f32), middle.astype(f32), low.astype(f32)


def fold_rows(values):
    return values.reshape(-1, 8, values.shape[-1]).sum(axis=0)


def column_sums(values_of, rows, valid):
    pixels = jnp.int32(0)
    total = None
    for row in rows:
        values = values_of(row)
        inside = row < valid
        pixels = pixels + jnp.where(inside, values.shape[0], 0)
        part = jnp.where(inside, fold_rows(values), 0.0)
        total = part if total is None else total + part
    total = jnp.sum(total, axis=0, keepdims=True)
    mean = total / jnp.maximum(pixels, 1).astype(f32)
    spread = None
    for row in rows:
        apart = values_of(row) - mean
        part = jnp.where(row < valid, fold_rows(apart * apart), 0.0)
        spread = part if spread is None else spread + part
    return pixels.astype(f32), total, jnp.sum(spread, axis=0, keepdims=True)


def merge_sums(one, two):
    pixels, other = jnp.maximum(one[0], 1.0), jnp.maximum(two[0], 1.0)
    apart = one[1] / pixels - two[1] / other
    weight = jnp.where(jnp.minimum(one[0], two[0]) > 0, pixels * other / (pixels + other), 0.0)
    return one[0] + two[0], one[1] + two[1], one[2] + two[2] + apart * apart * weight


def pack_stats(plan, sums, spreads):
    parts = list(split_three(jnp.concatenate(sums + spreads, axis=0)))
    padding = plan.stat_rows - 6 * plan.count
    if padding:
        parts.append(jnp.zeros((padding, plan.channels), f32))
    return jnp.concatenate(parts, axis=0).astype(bf16)


def fill_buffers(plan, stats, edge_of, columns, buf_refs):
    for k in range(plan.targets):
        buf_refs[k][0 : plan.stat_rows, :] = stats
        window = plan.window(k)
        for tile in range(plan.count):
            for edge in range(2):
                at = plan.row_base + (2 * tile + edge) * plan.width
                buf_refs[k][at : at + plan.width, :] = edge_of(tile, edge, window)
        for place, column in enumerate(columns):
            at = plan.col_base + place * plan.rows
            buf_refs[k][at : at + plan.rows, :] = column


def own_values(plan, ref):
    first = lax.axis_index(AXIS) * plan.count
    return [ref[first + tile] for tile in range(plan.count)]


def edges_kernel(plan, links_hbm, rows_hbm, image_hbm, x_hbm, links_ref, rows_ref, image_ref, *refs):
    buf_refs, (x_ref, sems) = refs[: plan.targets], refs[plan.targets :]
    tables = [
        pltpu.make_async_copy(source, target, sems.at[plan.count + place])
        for place, (source, target) in enumerate(
            ((rows_hbm, rows_ref), (links_hbm, links_ref), (image_hbm, image_ref))
        )
    ]
    copies = [pltpu.make_async_copy(x_hbm.at[tile], x_ref.at[tile], sems.at[tile]) for tile in range(plan.count)]
    for copy in tables[:1] + copies + tables[1:]:
        copy.start()
    for copy in tables:
        copy.wait()
    own_rows = own_values(plan, rows_ref)
    sums, spreads, columns = [], [], []
    for tile in range(plan.count):
        copies[tile].wait()
        _, total, spread = column_sums(lambda row: x_ref[tile, row].astype(f32), range(plan.rows), own_rows[tile])
        sums.append(total)
        spreads.append(spread)
        for column in (0, plan.cols - 1):
            picked = [x_ref[tile, row, column : column + 1, :].astype(f32) for row in range(plan.rows)]
            columns.append(jnp.concatenate(picked, axis=0).astype(bf16))

    def edge_of(tile, edge, window):
        return x_ref[tile, edge * (plan.rows - 1), window, :]

    fill_buffers(plan, pack_stats(plan, sums, spreads), edge_of, columns, buf_refs)


def group_total(values, group_width):
    lanes = values.shape[-1]
    lane = lax.broadcasted_iota(jnp.int32, values.shape, 1)
    step = 1
    while step < group_width:
        ahead = pltpu.roll(values, lanes - step, axis=1)
        behind = pltpu.roll(values, step, axis=1)
        values = values + jnp.where(lax.bitwise_and(lane, step) == 0, ahead, behind)
        step *= 2
    return values


class Held:
    def __init__(self, plan, bufs, held, part):
        self.plan = plan
        self.row_base, self.col_base = plan.row_base, plan.col_base
        self.held = bufs[0]
        if plan.direct:
            self.held = held
            self.row_base, self.col_base = 0, plan.stat_rows
            for slot in range(plan.slots):
                if part == "rows":
                    held[slot] = bufs[slot][plan.row_base : plan.col_base, :]
                else:
                    held[slot, 0 : plan.stat_rows, :] = bufs[slot][0 : plan.stat_rows, :]
                    held[slot, plan.stat_rows :, :] = bufs[slot][plan.col_base :, :]

    def locate(self, tile):
        tile = jnp.maximum(tile, 0)
        return self.plan.slot_of(lax.div(tile, self.plan.count)), lax.rem(tile, self.plan.count)

    def edge_row(self, tile, edge):
        slot, local = self.locate(tile)
        at = pl.multiple_of(self.row_base + (2 * local + edge) * self.plan.width, 16)
        return self.held[slot, pl.ds(at, self.plan.width), :]

    def edge_col(self, tile, edge):
        slot, local = self.locate(tile)
        at = pl.multiple_of(self.col_base + (2 * local + edge) * self.plan.rows, 16)
        return self.held[slot, pl.ds(at, self.plan.rows), :]


def held_scratch(plan, part):
    rows = plan.col_base - plan.row_base if part == "rows" else plan.buf_rows - plan.col_base + plan.stat_rows
    return pltpu.VMEM((plan.slots, rows, plan.channels) if plan.direct else (1, 16, plan.channels), bf16)


def buffer_inputs(plan, refs):
    inputs = plan.slots if plan.direct else 1
    return refs[:inputs], refs[inputs:]


def route_kernel(plan, links_ref, *refs):
    bufs, refs = buffer_inputs(plan, refs)
    send_refs, held = refs[:-1], Held(plan, bufs, refs[-1], "rows")
    for k in range(plan.parts):
        first = plan.target(k) * plan.count
        for tile in range(plan.count):
            for edge in range(2):
                at = (2 * tile + edge) * plan.width
                wanted = links_ref[edge, first + tile]
                send_refs[k][at : at + plan.width, :] = held.edge_row(wanted, 1 - edge)


def image_norms(plan, rows_ref, image_ref, held):
    count, channels = plan.count, plan.channels
    group_width = channels // G
    first = lax.axis_index(AXIS) * count
    partial = []
    for slot in range(plan.slots):
        raw = held[slot, 0 : plan.stat_rows, :].astype(f32)
        span = 2 * count
        partial.append(raw[0:span] + raw[span : 2 * span] + raw[2 * span : 3 * span])
    means, inverses = [], []
    for tile in range(count):
        image = image_ref[first + tile]
        weights, pixels = [], []
        area = jnp.int32(0)
        for slot in range(plan.slots):
            base = plan.device_of(slot) * count
            for other in range(count):
                same = image_ref[base + other] == image
                weights.append(jnp.where(same, 1.0, 0.0).astype(f32))
                amount = rows_ref[base + other] * plan.cols
                pixels.append(jnp.maximum(amount, 1).astype(f32))
                area = area + jnp.where(same, amount, 0)
        total = jnp.zeros((1, channels), f32)
        for slot in range(plan.slots):
            for other in range(count):
                total = total + weights[slot * count + other] * partial[slot][other : other + 1]
        amount = jnp.maximum(area * group_width, 1).astype(f32)
        mean = group_total(jnp.broadcast_to(total, (8, channels)), group_width)[0:1] / amount
        total = jnp.zeros((1, channels), f32)
        for slot in range(plan.slots):
            for other in range(count):
                place = slot * count + other
                apart = partial[slot][other : other + 1] / pixels[place] - mean
                spread = partial[slot][count + other : count + other + 1] + pixels[place] * apart * apart
                total = total + weights[place] * spread
        variance = group_total(jnp.broadcast_to(total, (8, channels)), group_width)[0:1] / amount
        means.append(mean)
        inverses.append(lax.rsqrt(variance + epsilon))
    return means, inverses


def halves(mean, inverse, gain_ref, shift_ref):
    scale = inverse * (gain_ref[...] * 0.5)
    shift = shift_ref[...] * 0.5

    def activate(values):
        half = (values.astype(f32) - mean) * scale + shift
        return half + half * jnp.tanh(half)

    return activate


def taps(act, before, after):
    cols = act.shape[0]
    pixel = lax.broadcasted_iota(jnp.int32, act.shape, 0)
    back = jnp.where(pixel == 0, before, pltpu.roll(act, 1, axis=0))
    ahead = jnp.where(pixel == cols - 1, after, pltpu.roll(act, cols - 1, axis=0))
    return [values.astype(bf16) for values in (back, act, ahead)]


def middle_kernel(plan, last, links_ref, rows_ref, image_ref, *refs):
    bufs, refs = buffer_inputs(plan, refs)
    x_ref, gain_ref, shift_ref, offset_ref, weight_ref = refs[:5]
    refs = refs[5:]
    ends_ref = residual_ref = None
    if last:
        (ends_ref, residual_ref), refs = refs[:2], refs[2:]
    out_ref, partial_ref, norm_ref, side_ref, held_ref, wide = refs[:6]
    refs = refs[6:]
    count, rows, cols, channels = plan.count, plan.rows, plan.cols, plan.channels
    held = Held(plan, bufs, held_ref, "rest")
    means, inverses = image_norms(plan, rows_ref, image_ref, held.held)
    first = lax.axis_index(AXIS) * count
    own_rows = own_values(plan, rows_ref)
    offset = offset_ref[...]
    norm_ref[0 : 2 * count, :] = jnp.concatenate(means + inverses, axis=0)
    copies = []
    for tile in range(count):
        valid = own_rows[tile]
        link = [links_ref[column, first + tile] for column in range(4)]
        activate = halves(means[tile], inverses[tile], gain_ref, shift_ref)
        left = jnp.where(link[2] >= 0, activate(held.edge_col(link[2], 1)), 0.0)
        right = jnp.where(link[3] >= 0, activate(held.edge_col(link[3], 0)), 0.0)
        corners = []
        for place in range(4):
            beside = links_ref[2 + place % 2, jnp.maximum(link[place // 2], 0)]
            beside = jnp.where(link[place // 2] >= 0, beside, -1)
            row = 0 if place // 2 else rows - 1
            corner = activate(held.edge_col(beside, 1 - place % 2))[row : row + 1]
            corners.append(jnp.where(beside >= 0, corner, 0.0))
        side_ref[8 * tile : 8 * tile + 4, :] = jnp.concatenate(corners, axis=0)

        depth = 3 * channels
        nothing = jnp.zeros((cols, depth), bf16)
        wide[tile, 0, :, 0:depth] = nothing
        wide[tile, rows // 2, :, depth : 2 * depth] = nothing
        for row in range(rows):
            if ends_ref is not None and row in (0, rows - 1):
                source = ends_ref[2 * tile + (row > 0)]
            else:
                source = x_ref[tile, row]
            act = jnp.where(row < valid, activate(source), 0.0)
            before = jnp.where(row < valid, left[row : row + 1], 0.0)
            after = jnp.where(row < valid, right[row : row + 1], 0.0)
            lane = ((row + 1) % 2) * depth
            for tap, values in enumerate(taps(act, before, after)):
                at = lane + tap * channels
                wide[tile, (row + 1) // 2, :, at : at + channels] = values

        pairs = rows // 2
        step = 2 if pairs % 2 == 0 else 1
        gathered = None
        for pair in range(0, pairs, step):
            upper = wide[tile, pair : pair + step].reshape(step * cols, 2 * depth)
            lower = wide[tile, pair + 1 : pair + step + 1].reshape(step * cols, 2 * depth)
            window = jnp.concatenate([upper, lower], axis=1)
            summed = jnp.dot(window, weight_ref[...], preferred_element_type=f32)
            inner = {}
            for row in range(2 * pair, 2 * (pair + step)):
                at, lane = (row // 2 - pair) * cols, (row % 2) * channels
                part = summed[at : at + cols, lane : lane + channels] + offset
                if last:
                    part = part + residual_ref[tile, row].astype(f32)
                if row in (0, rows - 1):
                    partial_ref[2 * tile + (row > 0)] = part
                    continue
                part = jnp.where(row < valid, part, 0.0).astype(bf16)
                if last:
                    refs[0][tile, row] = part
                else:
                    out_ref[tile, row] = part
                inner[row] = part.astype(f32)
            if last:
                band = pl.ds(min(inner), len(inner))
                sem = refs[1].at[tile * pairs + pair]
                copy = pltpu.make_async_copy(refs[0].at[tile, band], out_ref.at[tile, band], sem)
                copy.start()
                copies.append(copy)
            else:
                found = column_sums(lambda row: inner[row], sorted(inner), valid)
                gathered = found if gathered is None else merge_sums(gathered, found)
        if not last:
            norm_ref[(2 * count + tile) : (2 * count + tile) + 1, :] = gathered[1]
            norm_ref[(3 * count + tile) : (3 * count + tile) + 1, :] = gathered[2]
            for side, column in enumerate((0, cols - 1)):
                picked = [out_ref[tile, row, column : column + 1, :].astype(f32) for row in range(1, rows - 1)]
                at = 8 * count + (2 * tile + side) * rows
                side_ref[at + 1 : at + rows - 1, :] = jnp.concatenate(picked, axis=0)
    for copy in copies:
        copy.wait()


def ends_kernel(plan, last, links_ref, rows_ref, *refs):
    halo_refs, refs = refs[: plan.parts], refs[plan.parts :]
    partial_ref, norm_ref, side_ref, gain_ref, shift_ref, weight_ref = refs[:6]
    refs = refs[6:]
    count, rows, cols, channels = plan.count, plan.rows, plan.cols, plan.channels
    if last:
        _, out_ref, halo, ends_ref, sems = refs
    else:
        ends_ref, buf_refs, halo = refs[0], refs[1:-1], refs[-1]
    first = lax.axis_index(AXIS) * count
    own_rows = own_values(plan, rows_ref)
    for k in range(plan.parts):
        for place in range(2 * count):
            at = place * plan.width
            halo[place, plan.window(k), :] = halo_refs[k][at : at + plan.width, :]
    depth = 3 * channels
    copies, sums, spreads, columns = [], [], [], []
    for tile in range(count):
        valid = own_rows[tile]
        activate = halves(
            norm_ref[tile : tile + 1, :], norm_ref[count + tile : count + tile + 1, :], gain_ref, shift_ref
        )
        values = []
        for edge, row in enumerate((0, rows - 1)):
            place = 2 * tile + edge
            present = links_ref[edge, first + tile] >= 0
            act = jnp.where(present, activate(halo[place]), 0.0)
            at = 8 * tile + 2 * edge
            wide = jnp.concatenate(taps(act, side_ref[at : at + 1, :], side_ref[at + 1 : at + 2, :]), axis=1)
            weight = weight_ref[3 * edge * depth : (3 * edge + 1) * depth, edge * channels : (edge + 1) * channels]
            part = partial_ref[place] + jnp.dot(wide, weight, preferred_element_type=f32)
            result = jnp.where(row < valid, part, 0.0).astype(bf16)
            ends_ref[place] = result
            values.append(result.astype(f32))
            if last:
                copies.append(pltpu.make_async_copy(ends_ref.at[place], out_ref.at[tile, row], sems.at[place]))
                copies[-1].start()
        if last:
            continue
        found = column_sums(lambda row: values[row > 0], (0, rows - 1), valid)
        inner = (
            jnp.maximum((jnp.minimum(valid, rows - 1) - 1) * cols, 0).astype(f32),
            norm_ref[2 * count + tile : 2 * count + tile + 1, :],
            norm_ref[3 * count + tile : 3 * count + tile + 1, :],
        )
        _, total, spread = merge_sums(inner, found)
        sums.append(total)
        spreads.append(spread)
        line = lax.broadcasted_iota(jnp.int32, (rows, channels), 0)
        for side, column in enumerate((0, cols - 1)):
            at = 8 * count + (2 * tile + side) * rows
            picked = side_ref[at : at + rows, :]
            picked = jnp.where(line == 0, values[0][column : column + 1], picked)
            picked = jnp.where(line == rows - 1, values[1][column : column + 1], picked)
            columns.append(picked.astype(bf16))
    if not last:

        def edge_of(tile, edge, window):
            return ends_ref[2 * tile + edge, window, :]

        fill_buffers(plan, pack_stats(plan, sums, spreads), edge_of, columns, buf_refs)
    for copy in copies:
        copy.wait()


def paired_weights(kernel):
    upper = jnp.pad(kernel, ((0, 1), (0, 0), (0, 0), (0, 0)))
    lower = jnp.pad(kernel, ((1, 0), (0, 0), (0, 0), (0, 0)))
    both = jnp.concatenate([upper, lower], axis=-1)
    return both.reshape(-1, both.shape[-1])


def shards(
    feature_tiles,
    neighbours,
    valid_rows,
    tile_image,
    gain_one,
    shift_one,
    kernel_one,
    offset_one,
    gain_two,
    shift_two,
    kernel_two,
    offset_two,
    *,
    size,
):
    count, rows, cols, channels = feature_tiles.shape
    plan = Plan(size, count, rows, cols, channels)
    buf_shape = [jax.ShapeDtypeStruct((plan.buf_rows, channels), bf16)] * plan.targets
    limit = 24 * 1024 * 1024
    params = pltpu.CompilerParams(vmem_limit_bytes=limit)

    def swap(array, distance):
        return lax.ppermute(array, AXIS, [(i, i ^ distance) for i in range(size)])

    def spread(arrays):
        result = [arrays[0]]
        for k in range(1, len(arrays)):
            result.append(swap(arrays[k], 2 * k))
        return result

    def exchange(bufs):
        if not plan.direct:
            return [lax.all_gather(bufs[0], AXIS)]
        own = spread(bufs)
        return own + [swap(array, 1) for array in own]

    def shape(dims, dtype=f32):
        return jax.ShapeDtypeStruct(dims, dtype)

    partial_shape = shape((2 * count, cols, channels))
    norm_shape = shape((round_up(4 * count, 8), channels))
    side_shape = shape((8 * count + 2 * count * rows, channels))
    ends_shape = shape((2 * count, cols, channels), bf16)
    tiles_shape = shape(feature_tiles.shape, bf16)

    def stage(last, source, ends, bufs, gain, shift, kernel, offset):
        arrays = exchange(bufs)
        send = pl.pallas_call(
            functools.partial(route_kernel, plan),
            out_shape=[shape((2 * count * plan.width, channels), bf16)] * plan.parts,
            in_specs=[SMEM] + [VMEM] * len(arrays),
            out_specs=[VMEM] * plan.parts,
            scratch_shapes=[held_scratch(plan, "rows")],
            compiler_params=params,
        )(scalars[0], *arrays)
        halo = spread(send)
        weights = paired_weights(kernel)
        gain, shift, offset = gain[None], shift[None], offset[None]
        operands = arrays + [source, gain, shift, offset, weights] + ([ends, feature_tiles] if last else [])
        flops = 2 * count * rows * cols * 9 * channels * channels
        tiles, partial, norm, side = pl.pallas_call(
            functools.partial(middle_kernel, plan, last),
            out_shape=[tiles_shape, partial_shape, norm_shape, side_shape],
            in_specs=[SMEM] * 3 + [VMEM] * len(operands),
            out_specs=[HBM if last else VMEM] + [VMEM] * 3,
            scratch_shapes=[held_scratch(plan, "rest"), pltpu.VMEM((count, rows // 2 + 1, cols, 6 * channels), bf16)]
            + ([pltpu.VMEM(feature_tiles.shape, bf16), pltpu.SemaphoreType.DMA((count * rows // 2,))] if last else []),
            compiler_params=params,
            cost_estimate=pl.CostEstimate(flops=flops, bytes_accessed=4 * feature_tiles.size, transcendentals=0),
        )(*scalars, *operands)
        operands = halo + [partial, norm, side, gain, shift, weights]
        scratch = [pltpu.VMEM((2 * count, cols, channels), bf16)]
        if last:
            return pl.pallas_call(
                functools.partial(ends_kernel, plan, last),
                out_shape=tiles_shape,
                in_specs=[SMEM] * 2 + [VMEM] * len(operands) + [HBM],
                out_specs=HBM,
                input_output_aliases={2 + len(operands): 0},
                scratch_shapes=scratch + scratch + [pltpu.SemaphoreType.DMA((2 * count,))],
                compiler_params=params,
            )(*scalars[:2], *operands, tiles)
        ends, *bufs = pl.pallas_call(
            functools.partial(ends_kernel, plan, last),
            out_shape=[ends_shape] + buf_shape,
            in_specs=[SMEM] * 2 + [VMEM] * len(operands),
            out_specs=[VMEM] * (1 + plan.targets),
            scratch_shapes=scratch,
            compiler_params=params,
        )(*scalars[:2], *operands)
        return tiles, ends, bufs

    tables = (neighbours.T, valid_rows, tile_image)
    inputs = [pltpu.with_memory_space_constraint(array, pltpu.HBM) for array in (*tables, feature_tiles)]
    found = pl.pallas_call(
        functools.partial(edges_kernel, plan),
        out_shape=[pltpu.SMEM(table.shape, jnp.int32) for table in tables] + buf_shape,
        in_specs=[HBM] * 4,
        out_specs=[SMEM] * 3 + [VMEM] * plan.targets,
        scratch_shapes=[pltpu.VMEM(feature_tiles.shape, bf16), pltpu.SemaphoreType.DMA((count + 3,))],
        compiler_params=params,
        name="edges",
    )(*inputs)
    scalars, bufs = found[:3], found[3:]
    hidden, ends, bufs = stage(False, feature_tiles, None, bufs, gain_one, shift_one, kernel_one, offset_one)
    return stage(True, hidden, ends, bufs, gain_two, shift_two, kernel_two, offset_two)


def solution(mesh):
    in_specs = (
        P(("rep", "tile"), None, None, None),
        P("rep", None),
        P("rep"),
        P("rep"),
        P(),
        P(),
        P(),
        P(),
        P(),
        P(),
        P(),
        P(),
    )
    out_specs = P(("rep", "tile"), None, None, None)

    def body(*args):
        return shards(*args, size=mesh.shape[AXIS])

    return jax.shard_map(body, mesh=mesh, in_specs=in_specs, out_specs=out_specs, check_vma=False)
```

```python
import functools

import jax
import jax.numpy as jnp
from jax import lax
from jax.experimental import pallas as pl
from jax.experimental.pallas import tpu as pltpu
from jax.sharding import PartitionSpec as P


G = 32
AXIS = "tile"
epsilon = 1e-06
f32 = jnp.float32
bf16 = jnp.bfloat16


VMEM = pl.BlockSpec(memory_space=pltpu.VMEM)
SMEM = pl.BlockSpec(memory_space=pltpu.SMEM)
HBM = pl.BlockSpec(memory_space=pltpu.HBM)


def round_up(value, step):
    return -(-value // step) * step


class Plan:
    def __init__(self, size, count, rows, cols, channels):
        self.size, self.count, self.rows, self.cols, self.channels = size, count, rows, cols, channels
        chips = size // 2
        self.direct = size % 2 == 0 and chips in (2, 4, 8) and cols % 32 == 0
        self.targets = chips if self.direct else 1
        self.parts = 2 if self.direct else 1
        self.width = cols // self.parts
        self.stat_rows = round_up(6 * count, 16)
        self.row_base = self.stat_rows
        self.col_base = self.row_base + 2 * count * self.width
        self.buf_rows = self.col_base + 2 * count * rows
        self.slots = size

    def place(self):
        index = lax.axis_index(AXIS)
        return lax.div(index, 2), lax.rem(index, 2)

    def window(self, k):
        if not self.direct:
            return pl.ds(0, self.width)
        part = lax.bitwise_and(lax.bitwise_xor(self.place()[0], k), 1)
        return pl.ds(pl.multiple_of(part * self.width, 16), self.width)

    def slot_of(self, device):
        if not self.direct:
            return device
        chip, core = self.place()
        other = lax.bitwise_xor(lax.rem(device, 2), core)
        return other * self.targets + lax.bitwise_xor(lax.div(device, 2), chip)

    def device_of(self, slot):
        if not self.direct:
            return slot
        chip, core = self.place()
        return lax.bitwise_xor(chip, slot % self.targets) * 2 + lax.bitwise_xor(core, slot // self.targets)

    def target(self, k):
        if not self.direct:
            return lax.axis_index(AXIS)
        chip, core = self.place()
        return lax.bitwise_xor(chip, k) * 2 + core


def split_three(values):
    high = values.astype(bf16)
    rest = values - high.astype(f32)
    middle = rest.astype(bf16)
    low = (rest - middle.astype(f32)).astype(bf16)
    return high.astype(f32), middle.astype(f32), low.astype(f32)


def fold_rows(values):
    return values.reshape(-1, 8, values.shape[-1]).sum(axis=0)


def column_sums(values_of, rows, valid):
    rows = list(rows)
    first = values_of(rows[0])
    pivot = jnp.sum(fold_rows(first), axis=0, keepdims=True) * (1.0 / first.shape[0])
    pixels = jnp.int32(0)
    total = spread = None
    for row in rows:
        apart = values_of(row) - pivot
        inside = row < valid
        pixels = pixels + jnp.where(inside, apart.shape[0], 0)
        part = jnp.where(inside, fold_rows(apart), 0.0)
        square = jnp.where(inside, fold_rows(apart * apart), 0.0)
        total = part if total is None else total + part
        spread = square if spread is None else spread + square
    total = jnp.sum(total, axis=0, keepdims=True)
    spread = jnp.sum(spread, axis=0, keepdims=True)
    pixels = pixels.astype(f32)
    spread = jnp.maximum(spread - total * (total / jnp.maximum(pixels, 1.0)), 0.0)
    return pixels, total + pixels * pivot, spread


def merge_sums(one, two):
    pixels, other = jnp.maximum(one[0], 1.0), jnp.maximum(two[0], 1.0)
    apart = one[1] / pixels - two[1] / other
    weight = jnp.where(jnp.minimum(one[0], two[0]) > 0, pixels * other / (pixels + other), 0.0)
    return one[0] + two[0], one[1] + two[1], one[2] + two[2] + apart * apart * weight


def pack_stats(plan, sums, spreads):
    parts = list(split_three(jnp.concatenate(sums + spreads, axis=0)))
    padding = plan.stat_rows - 6 * plan.count
    if padding:
        parts.append(jnp.zeros((padding, plan.channels), f32))
    return jnp.concatenate(parts, axis=0).astype(bf16)


def fill_buffers(plan, stats, edge_of, columns, buf_refs):
    for k in range(plan.targets):
        buf_refs[k][0 : plan.stat_rows, :] = stats
        window = plan.window(k)
        for tile in range(plan.count):
            for edge in range(2):
                at = plan.row_base + (2 * tile + edge) * plan.width
                buf_refs[k][at : at + plan.width, :] = edge_of(tile, edge, window)
        for place, column in enumerate(columns):
            at = plan.col_base + place * plan.rows
            buf_refs[k][at : at + plan.rows, :] = column


def own_values(plan, ref):
    first = lax.axis_index(AXIS) * plan.count
    return [ref[first + tile] for tile in range(plan.count)]


def edges_kernel(plan, links_hbm, rows_hbm, image_hbm, x_hbm, links_ref, rows_ref, image_ref, *refs):
    x_ref, buf_refs, sems = refs[0], refs[1:-1], refs[-1]
    tables = [
        pltpu.make_async_copy(source, target, sems.at[plan.count + place])
        for place, (source, target) in enumerate(
            ((rows_hbm, rows_ref), (links_hbm, links_ref), (image_hbm, image_ref))
        )
    ]
    copies = [pltpu.make_async_copy(x_hbm.at[tile], x_ref.at[tile], sems.at[tile]) for tile in range(plan.count)]
    for copy in tables[:1] + copies + tables[1:]:
        copy.start()
    tables[0].wait()
    own_rows = own_values(plan, rows_ref)
    sums, spreads, columns = [], [], []
    for tile in range(plan.count):
        copies[tile].wait()
        _, total, spread = column_sums(lambda row: x_ref[tile, row].astype(f32), range(plan.rows), own_rows[tile])
        sums.append(total)
        spreads.append(spread)
        for column in (0, plan.cols - 1):
            picked = [x_ref[tile, row, column : column + 1, :].astype(f32) for row in range(plan.rows)]
            columns.append(jnp.concatenate(picked, axis=0).astype(bf16))

    def edge_of(tile, edge, window):
        return x_ref[tile, edge * (plan.rows - 1), window, :]

    fill_buffers(plan, pack_stats(plan, sums, spreads), edge_of, columns, buf_refs)
    for copy in tables[1:]:
        copy.wait()


def group_total(values, group_width):
    lanes = values.shape[-1]
    lane = lax.broadcasted_iota(jnp.int32, values.shape, 1)
    step = 1
    while step < group_width:
        ahead = pltpu.roll(values, lanes - step, axis=1)
        behind = pltpu.roll(values, step, axis=1)
        values = values + jnp.where(lax.bitwise_and(lane, step) == 0, ahead, behind)
        step *= 2
    return values


class Held:
    def __init__(self, plan, bufs, held, part):
        self.plan = plan
        self.row_base, self.col_base = plan.row_base, plan.col_base
        self.held = bufs[0]
        if plan.direct:
            self.held = held
            self.row_base, self.col_base = 0, plan.stat_rows
            for slot in range(plan.slots):
                if part == "rows":
                    held[slot] = bufs[slot][plan.row_base : plan.col_base, :]
                else:
                    held[slot, 0 : plan.stat_rows, :] = bufs[slot][0 : plan.stat_rows, :]
                    held[slot, plan.stat_rows :, :] = bufs[slot][plan.col_base :, :]

    def locate(self, tile):
        tile = jnp.maximum(tile, 0)
        return self.plan.slot_of(lax.div(tile, self.plan.count)), lax.rem(tile, self.plan.count)

    def edge_row(self, tile, edge):
        slot, local = self.locate(tile)
        at = pl.multiple_of(self.row_base + (2 * local + edge) * self.plan.width, 16)
        return self.held[slot, pl.ds(at, self.plan.width), :]

    def edge_col(self, tile, edge):
        slot, local = self.locate(tile)
        at = pl.multiple_of(self.col_base + (2 * local + edge) * self.plan.rows, 16)
        return self.held[slot, pl.ds(at, self.plan.rows), :]


def held_scratch(plan, part):
    rows = plan.col_base - plan.row_base if part == "rows" else plan.buf_rows - plan.col_base + plan.stat_rows
    return pltpu.VMEM((plan.slots, rows, plan.channels) if plan.direct else (1, 16, plan.channels), bf16)


def buffer_inputs(plan, refs):
    inputs = plan.slots if plan.direct else 1
    return refs[:inputs], refs[inputs:]


def route_kernel(plan, links_ref, *refs):
    bufs, refs = buffer_inputs(plan, refs)
    send_refs, held = refs[:-1], Held(plan, bufs, refs[-1], "rows")
    for k in range(plan.parts):
        first = plan.target(k) * plan.count
        for tile in range(plan.count):
            for edge in range(2):
                at = (2 * tile + edge) * plan.width
                wanted = links_ref[edge, first + tile]
                send_refs[k][at : at + plan.width, :] = held.edge_row(wanted, 1 - edge)


def image_norms(plan, rows_ref, image_ref, held):
    count, channels = plan.count, plan.channels
    group_width = channels // G
    first = lax.axis_index(AXIS) * count
    partial = []
    for slot in range(plan.slots):
        raw = held[slot, 0 : plan.stat_rows, :].astype(f32)
        span = 2 * count
        partial.append(raw[0:span] + raw[span : 2 * span] + raw[2 * span : 3 * span])
    means, inverses = [], []
    for tile in range(count):
        image = image_ref[first + tile]
        weights, pixels = [], []
        area = jnp.int32(0)
        for slot in range(plan.slots):
            base = plan.device_of(slot) * count
            for other in range(count):
                same = image_ref[base + other] == image
                weights.append(jnp.where(same, 1.0, 0.0).astype(f32))
                amount = rows_ref[base + other] * plan.cols
                pixels.append(jnp.maximum(amount, 1).astype(f32))
                area = area + jnp.where(same, amount, 0)
        total = jnp.zeros((1, channels), f32)
        for slot in range(plan.slots):
            for other in range(count):
                total = total + weights[slot * count + other] * partial[slot][other : other + 1]
        amount = jnp.maximum(area * group_width, 1).astype(f32)
        mean = group_total(jnp.broadcast_to(total, (8, channels)), group_width)[0:1] / amount
        total = jnp.zeros((1, channels), f32)
        for slot in range(plan.slots):
            for other in range(count):
                place = slot * count + other
                apart = partial[slot][other : other + 1] / pixels[place] - mean
                spread = partial[slot][count + other : count + other + 1] + pixels[place] * apart * apart
                total = total + weights[place] * spread
        variance = group_total(jnp.broadcast_to(total, (8, channels)), group_width)[0:1] / amount
        means.append(mean)
        inverses.append(lax.rsqrt(variance + epsilon))
    return means, inverses


def halves(mean, inverse, gain_ref, shift_ref):
    scale = inverse * (gain_ref[...] * 0.5)
    shift = shift_ref[...] * 0.5

    def activate(values):
        half = (values.astype(f32) - mean) * scale + shift
        return half + half * jnp.tanh(half)

    return activate


def taps(act, before, after):
    cols = act.shape[0]
    pixel = lax.broadcasted_iota(jnp.int32, act.shape, 0)
    back = jnp.where(pixel == 0, before, pltpu.roll(act, 1, axis=0))
    ahead = jnp.where(pixel == cols - 1, after, pltpu.roll(act, cols - 1, axis=0))
    return [values.astype(bf16) for values in (back, act, ahead)]


def middle_kernel(plan, last, links_ref, rows_ref, image_ref, *refs):
    bufs, refs = buffer_inputs(plan, refs)
    x_ref, gain_ref, shift_ref, offset_ref, weight_ref = refs[:5]
    refs = refs[5:]
    ends_ref = residual_ref = None
    if last:
        (ends_ref, residual_ref), refs = refs[:2], refs[2:]
    if last:
        out_ref, partial_ref, norm_ref, side_ref, rest_ref, held_ref, wide, tiles_ref, sems = refs
    else:
        tiles_ref, partial_ref, norm_ref, side_ref, held_ref, wide = refs
    count, rows, cols, channels = plan.count, plan.rows, plan.cols, plan.channels
    held = Held(plan, bufs, held_ref, "rest")
    means, inverses = image_norms(plan, rows_ref, image_ref, held.held)
    first = lax.axis_index(AXIS) * count
    own_rows = own_values(plan, rows_ref)
    offset = offset_ref[...]
    norm_ref[0 : 2 * count, :] = jnp.concatenate(means + inverses, axis=0)
    copies = []
    for tile in range(count):
        valid = own_rows[tile]
        link = [links_ref[column, first + tile] for column in range(4)]
        activate = halves(means[tile], inverses[tile], gain_ref, shift_ref)
        left = jnp.where(link[2] >= 0, activate(held.edge_col(link[2], 1)), 0.0)
        right = jnp.where(link[3] >= 0, activate(held.edge_col(link[3], 0)), 0.0)
        corners = []
        for place in range(4):
            beside = links_ref[2 + place % 2, jnp.maximum(link[place // 2], 0)]
            beside = jnp.where(link[place // 2] >= 0, beside, -1)
            row = 0 if place // 2 else rows - 1
            corner = activate(held.edge_col(beside, 1 - place % 2))[row : row + 1]
            corners.append(jnp.where(beside >= 0, corner, 0.0))
        side_ref[8 * tile : 8 * tile + 4, :] = jnp.concatenate(corners, axis=0)

        depth = 3 * channels
        nothing = jnp.zeros((cols, depth), bf16)
        wide[tile, 0, :, 0:depth] = nothing
        wide[tile, rows // 2, :, depth : 2 * depth] = nothing
        for row in range(rows):
            if ends_ref is not None and row in (0, rows - 1):
                source = ends_ref[2 * tile + (row > 0)]
            else:
                source = x_ref[tile, row]
            act = jnp.where(row < valid, activate(source), 0.0)
            before = jnp.where(row < valid, left[row : row + 1], 0.0)
            after = jnp.where(row < valid, right[row : row + 1], 0.0)
            lane = ((row + 1) % 2) * depth
            for tap, values in enumerate(taps(act, before, after)):
                at = lane + tap * channels
                wide[tile, (row + 1) // 2, :, at : at + channels] = values

        pairs = rows // 2
        step = 1
        gathered = None
        for pair in range(0, pairs, step):
            upper = wide[tile, pair : pair + step].reshape(step * cols, 2 * depth)
            lower = wide[tile, pair + 1 : pair + step + 1].reshape(step * cols, 2 * depth)
            window = jnp.concatenate([upper, lower], axis=1)
            summed = jnp.dot(window, weight_ref[...], preferred_element_type=f32)
            inner = {}
            for row in range(2 * pair, 2 * (pair + step)):
                at, lane = (row // 2 - pair) * cols, (row % 2) * channels
                part = summed[at : at + cols, lane : lane + channels] + offset
                if last:
                    part = part + residual_ref[tile, row].astype(f32)
                if row in (0, rows - 1):
                    partial_ref[2 * tile + (row > 0)] = part
                    continue
                part = jnp.where(row < valid, part, 0.0).astype(bf16)
                if last and tile == count - 1:
                    rest_ref[row - 1] = part
                    continue
                tiles_ref[tile, row] = part
                inner[row] = part.astype(f32)
            if last:
                if not inner:
                    continue
                band = pl.ds(min(inner), len(inner))
                sem = sems.at[tile * pairs + pair]
                copy = pltpu.make_async_copy(tiles_ref.at[tile, band], out_ref.at[tile, band], sem)
                copy.start()
                copies.append(copy)
            else:
                found = column_sums(lambda row: inner[row], sorted(inner), valid)
                gathered = found if gathered is None else merge_sums(gathered, found)
        if not last:
            norm_ref[(2 * count + tile) : (2 * count + tile) + 1, :] = gathered[1]
            norm_ref[(3 * count + tile) : (3 * count + tile) + 1, :] = gathered[2]
            for side, column in enumerate((0, cols - 1)):
                picked = [tiles_ref[tile, row, column : column + 1, :].astype(f32) for row in range(1, rows - 1)]
                at = 8 * count + (2 * tile + side) * rows
                side_ref[at + 1 : at + rows - 1, :] = jnp.concatenate(picked, axis=0)
    for copy in copies:
        copy.wait()


def ends_kernel(plan, last, links_ref, rows_ref, *refs):
    halo_refs, refs = refs[: plan.parts], refs[plan.parts :]
    partial_ref, norm_ref, side_ref, gain_ref, shift_ref, weight_ref = refs[:6]
    refs = refs[6:]
    count, rows, cols, channels = plan.count, plan.rows, plan.cols, plan.channels
    if last:
        rest_ref, _, out_ref, halo, ends_ref, sems = refs
    else:
        ends_ref, buf_refs, halo = refs[0], refs[1:-1], refs[-1]
    first = lax.axis_index(AXIS) * count
    own_rows = own_values(plan, rows_ref)
    for k in range(plan.parts):
        for place in range(2 * count):
            at = place * plan.width
            halo[place, plan.window(k), :] = halo_refs[k][at : at + plan.width, :]
    depth = 3 * channels
    copies, sums, spreads, columns = [], [], [], []
    if last:
        target = out_ref.at[count - 1, pl.ds(1, rows - 2)]
        copies.append(pltpu.make_async_copy(rest_ref, target, sems.at[2 * count]))
        copies[-1].start()
    for tile in range(count):
        valid = own_rows[tile]
        activate = halves(
            norm_ref[tile : tile + 1, :], norm_ref[count + tile : count + tile + 1, :], gain_ref, shift_ref
        )
        values = []
        for edge, row in enumerate((0, rows - 1)):
            place = 2 * tile + edge
            present = links_ref[edge, first + tile] >= 0
            act = jnp.where(present, activate(halo[place]), 0.0)
            at = 8 * tile + 2 * edge
            wide = jnp.concatenate(taps(act, side_ref[at : at + 1, :], side_ref[at + 1 : at + 2, :]), axis=1)
            weight = weight_ref[3 * edge * depth : (3 * edge + 1) * depth, edge * channels : (edge + 1) * channels]
            part = partial_ref[place] + jnp.dot(wide, weight, preferred_element_type=f32)
            result = jnp.where(row < valid, part, 0.0).astype(bf16)
            ends_ref[place] = result
            values.append(result.astype(f32))
            if last:
                copies.append(pltpu.make_async_copy(ends_ref.at[place], out_ref.at[tile, row], sems.at[place]))
                copies[-1].start()
        if last:
            continue
        found = column_sums(lambda row: values[row > 0], (0, rows - 1), valid)
        inner = (
            jnp.maximum((jnp.minimum(valid, rows - 1) - 1) * cols, 0).astype(f32),
            norm_ref[2 * count + tile : 2 * count + tile + 1, :],
            norm_ref[3 * count + tile : 3 * count + tile + 1, :],
        )
        _, total, spread = merge_sums(inner, found)
        sums.append(total)
        spreads.append(spread)
        line = lax.broadcasted_iota(jnp.int32, (rows, channels), 0)
        for side, column in enumerate((0, cols - 1)):
            at = 8 * count + (2 * tile + side) * rows
            picked = side_ref[at : at + rows, :]
            picked = jnp.where(line == 0, values[0][column : column + 1], picked)
            picked = jnp.where(line == rows - 1, values[1][column : column + 1], picked)
            columns.append(picked.astype(bf16))
    if not last:

        def edge_of(tile, edge, window):
            return ends_ref[2 * tile + edge, window, :]

        fill_buffers(plan, pack_stats(plan, sums, spreads), edge_of, columns, buf_refs)
    for copy in copies:
        copy.wait()


def paired_weights(kernel):
    upper = jnp.pad(kernel, ((0, 1), (0, 0), (0, 0), (0, 0)))
    lower = jnp.pad(kernel, ((1, 0), (0, 0), (0, 0), (0, 0)))
    both = jnp.concatenate([upper, lower], axis=-1)
    return both.reshape(-1, both.shape[-1])


def shards(
    feature_tiles,
    neighbours,
    valid_rows,
    tile_image,
    gain_one,
    shift_one,
    kernel_one,
    offset_one,
    gain_two,
    shift_two,
    kernel_two,
    offset_two,
    *,
    size,
):
    count, rows, cols, channels = feature_tiles.shape
    plan = Plan(size, count, rows, cols, channels)
    buf_shape = [jax.ShapeDtypeStruct((plan.buf_rows, channels), bf16)] * plan.targets
    limit = 24 * 1024 * 1024
    params = pltpu.CompilerParams(vmem_limit_bytes=limit)

    def swap(array, distance):
        return lax.ppermute(array, AXIS, [(i, i ^ distance) for i in range(size)])

    def spread(arrays):
        result = [arrays[0]]
        for k in range(1, len(arrays)):
            result.append(swap(arrays[k], 2 * k))
        return result

    def exchange(bufs):
        if not plan.direct:
            return [lax.all_gather(bufs[0], AXIS)]
        own = spread(bufs)
        return own + [swap(array, 1) for array in own]

    def shape(dims, dtype=f32):
        return jax.ShapeDtypeStruct(dims, dtype)

    partial_shape = shape((2 * count, cols, channels))
    norm_shape = shape((round_up(4 * count, 8), channels))
    side_shape = shape((8 * count + 2 * count * rows, channels))
    ends_shape = shape((2 * count, cols, channels), bf16)
    tiles_shape = shape(feature_tiles.shape, bf16)

    def stage(last, source, ends, bufs, gain, shift, kernel, offset):
        arrays = exchange(bufs)
        send = pl.pallas_call(
            functools.partial(route_kernel, plan),
            out_shape=[shape((2 * count * plan.width, channels), bf16)] * plan.parts,
            in_specs=[SMEM] + [VMEM] * len(arrays),
            out_specs=[VMEM] * plan.parts,
            scratch_shapes=[held_scratch(plan, "rows")],
            compiler_params=params,
        )(scalars[0], *arrays)
        halo = spread(send)
        weights = paired_weights(kernel)
        gain, shift, offset = gain[None], shift[None], offset[None]
        operands = arrays + [source, gain, shift, offset, weights] + ([ends, features] if last else [])
        flops = 2 * count * rows * cols * 9 * channels * channels
        tiles, partial, norm, side, *rest = pl.pallas_call(
            functools.partial(middle_kernel, plan, last),
            out_shape=[tiles_shape, partial_shape, norm_shape, side_shape] + [shape((rows - 2, cols, channels), bf16)] * last,
            in_specs=[SMEM] * 3 + [VMEM] * len(operands),
            out_specs=[HBM if last else VMEM] + [VMEM] * (3 + last),
            scratch_shapes=[held_scratch(plan, "rest"), pltpu.VMEM((count, rows // 2 + 1, cols, 6 * channels), bf16)]
            + ([pltpu.VMEM(feature_tiles.shape, bf16), pltpu.SemaphoreType.DMA((count * rows // 2,))] if last else []),
            compiler_params=params,
            cost_estimate=pl.CostEstimate(flops=flops, bytes_accessed=4 * feature_tiles.size, transcendentals=0),
        )(*scalars, *operands)
        operands = halo + [partial, norm, side, gain, shift, weights] + rest
        scratch = [pltpu.VMEM((2 * count, cols, channels), bf16)]
        if last:
            return pl.pallas_call(
                functools.partial(ends_kernel, plan, last),
                out_shape=tiles_shape,
                in_specs=[SMEM] * 2 + [VMEM] * len(operands) + [HBM],
                out_specs=HBM,
                input_output_aliases={2 + len(operands): 0},
                scratch_shapes=scratch + scratch + [pltpu.SemaphoreType.DMA((2 * count + 1,))],
                compiler_params=params,
            )(*scalars[:2], *operands, tiles)
        ends, *bufs = pl.pallas_call(
            functools.partial(ends_kernel, plan, last),
            out_shape=[ends_shape] + buf_shape,
            in_specs=[SMEM] * 2 + [VMEM] * len(operands),
            out_specs=[VMEM] * (1 + plan.targets),
            scratch_shapes=scratch,
            compiler_params=params,
        )(*scalars[:2], *operands)
        return tiles, ends, bufs

    tables = (neighbours.T, valid_rows, tile_image)
    inputs = [pltpu.with_memory_space_constraint(array, pltpu.HBM) for array in (*tables, feature_tiles)]
    found = pl.pallas_call(
        functools.partial(edges_kernel, plan),
        out_shape=[pltpu.SMEM(table.shape, jnp.int32) for table in tables] + [tiles_shape] + buf_shape,
        in_specs=[HBM] * 4,
        out_specs=[SMEM] * 3 + [VMEM] * (1 + plan.targets),
        scratch_shapes=[pltpu.SemaphoreType.DMA((count + 3,))],
        compiler_params=params,
        name="edges",
    )(*inputs)
    scalars, features, bufs = found[:3], found[3], found[4:]
    hidden, ends, bufs = stage(False, features, None, bufs, gain_one, shift_one, kernel_one, offset_one)
    return stage(True, hidden, ends, bufs, gain_two, shift_two, kernel_two, offset_two)


def solution(mesh):
    in_specs = (
        P(("rep", "tile"), None, None, None),
        P("rep", None),
        P("rep"),
        P("rep"),
        P(),
        P(),
        P(),
        P(),
        P(),
        P(),
        P(),
        P(),
    )
    out_specs = P(("rep", "tile"), None, None, None)

    def body(*args):
        return shards(*args, size=mesh.shape[AXIS])

    return jax.shard_map(body, mesh=mesh, in_specs=in_specs, out_specs=out_specs, check_vma=False)
```

```python
import functools

import jax
import jax.numpy as jnp
from jax import lax
from jax.experimental import pallas as pl
from jax.experimental.pallas import tpu as pltpu
from jax.sharding import PartitionSpec as P


G = 32
AXIS = "tile"
epsilon = 1e-06
f32 = jnp.float32
bf16 = jnp.bfloat16


VMEM = pl.BlockSpec(memory_space=pltpu.VMEM)
SMEM = pl.BlockSpec(memory_space=pltpu.SMEM)
HBM = pl.BlockSpec(memory_space=pltpu.HBM)


def round_up(value, step):
    return -(-value // step) * step


class Plan:
    def __init__(self, size, count, rows, cols, channels):
        self.size, self.count, self.rows, self.cols, self.channels = size, count, rows, cols, channels
        chips = size // 2
        self.direct = size % 2 == 0 and chips in (2, 4, 8) and cols % 32 == 0
        self.targets = chips if self.direct else 1
        self.parts = 2 if self.direct else 1
        self.width = cols // self.parts
        self.stat_rows = round_up(6 * count, 16)
        self.row_base = self.stat_rows
        self.col_base = self.row_base + 2 * count * self.width
        self.buf_rows = self.col_base + 2 * count * rows
        self.slots = size

    def place(self):
        index = lax.axis_index(AXIS)
        return lax.div(index, 2), lax.rem(index, 2)

    def window(self, k):
        if not self.direct:
            return pl.ds(0, self.width)
        part = lax.bitwise_and(lax.bitwise_xor(self.place()[0], k), 1)
        return pl.ds(pl.multiple_of(part * self.width, 16), self.width)

    def slot_of(self, device):
        if not self.direct:
            return device
        chip, core = self.place()
        other = lax.bitwise_xor(lax.rem(device, 2), core)
        return other * self.targets + lax.bitwise_xor(lax.div(device, 2), chip)

    def device_of(self, slot):
        if not self.direct:
            return slot
        chip, core = self.place()
        return lax.bitwise_xor(chip, slot % self.targets) * 2 + lax.bitwise_xor(core, slot // self.targets)

    def target(self, k):
        if not self.direct:
            return lax.axis_index(AXIS)
        chip, core = self.place()
        return lax.bitwise_xor(chip, k) * 2 + core


def split_three(values):
    high = values.astype(bf16)
    rest = values - high.astype(f32)
    middle = rest.astype(bf16)
    low = (rest - middle.astype(f32)).astype(bf16)
    return high.astype(f32), middle.astype(f32), low.astype(f32)


def fold_rows(values):
    return values.reshape(-1, 8, values.shape[-1]).sum(axis=0)


def mean_of(values):
    return jnp.sum(fold_rows(values), axis=0, keepdims=True) * (1.0 / values.shape[0])


def row_sums(values_of, rows, pivot):
    found = []
    for row in rows:
        apart = values_of(row) - pivot
        found.append((row, fold_rows(apart), fold_rows(apart * apart)))
    return found


def masked_sums(width, pivot, found, valid):
    pixels = jnp.int32(0)
    total = spread = None
    for row, part, square in found:
        inside = row < valid
        pixels = pixels + jnp.where(inside, width, 0)
        part, square = jnp.where(inside, part, 0.0), jnp.where(inside, square, 0.0)
        total = part if total is None else total + part
        spread = square if spread is None else spread + square
    total = jnp.sum(total, axis=0, keepdims=True)
    spread = jnp.sum(spread, axis=0, keepdims=True)
    pixels = pixels.astype(f32)
    spread = jnp.maximum(spread - total * (total / jnp.maximum(pixels, 1.0)), 0.0)
    return pixels, total + pixels * pivot, spread


def column_sums(values_of, rows, valid):
    rows = list(rows)
    first = values_of(rows[0])
    pivot = mean_of(first)
    return masked_sums(first.shape[0], pivot, row_sums(values_of, rows, pivot), valid)


def merge_sums(one, two):
    pixels, other = jnp.maximum(one[0], 1.0), jnp.maximum(two[0], 1.0)
    apart = one[1] / pixels - two[1] / other
    weight = jnp.where(jnp.minimum(one[0], two[0]) > 0, pixels * other / (pixels + other), 0.0)
    return one[0] + two[0], one[1] + two[1], one[2] + two[2] + apart * apart * weight


def pack_stats(plan, sums, spreads):
    parts = list(split_three(jnp.concatenate(sums + spreads, axis=0)))
    padding = plan.stat_rows - 6 * plan.count
    if padding:
        parts.append(jnp.zeros((padding, plan.channels), f32))
    return jnp.concatenate(parts, axis=0).astype(bf16)


def fill_buffers(plan, stats, edge_of, columns, buf_refs):
    for k in range(plan.targets):
        buf_refs[k][0 : plan.stat_rows, :] = stats
        window = plan.window(k)
        for tile in range(plan.count):
            for edge in range(2):
                at = plan.row_base + (2 * tile + edge) * plan.width
                buf_refs[k][at : at + plan.width, :] = edge_of(tile, edge, window)
        for place, column in enumerate(columns):
            at = plan.col_base + place * plan.rows
            buf_refs[k][at : at + plan.rows, :] = column


def own_values(plan, ref):
    first = lax.axis_index(AXIS) * plan.count
    return [ref[first + tile] for tile in range(plan.count)]


def edges_kernel(plan, links_hbm, rows_hbm, image_hbm, x_hbm, links_ref, rows_ref, image_ref, *refs):
    x_ref, buf_refs, sems = refs[0], refs[1:-1], refs[-1]
    tables = [
        pltpu.make_async_copy(source, target, sems.at[place])
        for place, (source, target) in enumerate(
            ((rows_hbm, rows_ref), (links_hbm, links_ref), (image_hbm, image_ref))
        )
    ]
    bands = 4
    height = plan.rows // bands
    copies = {}
    for tile in range(plan.count):
        for band in range(bands):
            window = pl.ds(band * height, height)
            sem = sems.at[3 + tile * bands + band]
            copies[tile, band] = pltpu.make_async_copy(x_hbm.at[tile, window], x_ref.at[tile, window], sem)
    for copy in [tables[0], *copies.values(), *tables[1:]]:
        copy.start()
    found, columns = [], []
    for tile in range(plan.count):
        pieces = []
        for band in range(bands):
            copies[tile, band].wait()
            rows = range(band * height, (band + 1) * height)
            if band == 0:
                pivot = mean_of(x_ref[tile, 0].astype(f32))
            pieces += row_sums(lambda row: x_ref[tile, row].astype(f32), rows, pivot)
        found.append((plan.cols, pivot, pieces))
        for column in (0, plan.cols - 1):
            picked = [x_ref[tile, row, column : column + 1, :].astype(f32) for row in range(plan.rows)]
            columns.append(jnp.concatenate(picked, axis=0).astype(bf16))
    tables[0].wait()
    own_rows = own_values(plan, rows_ref)
    sums, spreads = [], []
    for tile in range(plan.count):
        _, total, spread = masked_sums(*found[tile], own_rows[tile])
        sums.append(total)
        spreads.append(spread)

    def edge_of(tile, edge, window):
        return x_ref[tile, edge * (plan.rows - 1), window, :]

    fill_buffers(plan, pack_stats(plan, sums, spreads), edge_of, columns, buf_refs)
    for copy in tables[1:]:
        copy.wait()


def group_total(values, group_width):
    lanes = values.shape[-1]
    lane = lax.broadcasted_iota(jnp.int32, values.shape, 1)
    step = 1
    while step < group_width:
        ahead = pltpu.roll(values, lanes - step, axis=1)
        behind = pltpu.roll(values, step, axis=1)
        values = values + jnp.where(lax.bitwise_and(lane, step) == 0, ahead, behind)
        step *= 2
    return values


class Held:
    def __init__(self, plan, bufs, held, part):
        self.plan = plan
        self.row_base, self.col_base = plan.row_base, plan.col_base
        self.held = bufs[0]
        if plan.direct:
            self.held = held
            self.row_base, self.col_base = 0, plan.stat_rows
            for slot in range(plan.slots):
                if part == "rows":
                    held[slot] = bufs[slot][plan.row_base : plan.col_base, :]
                else:
                    held[slot, 0 : plan.stat_rows, :] = bufs[slot][0 : plan.stat_rows, :]
                    held[slot, plan.stat_rows :, :] = bufs[slot][plan.col_base :, :]

    def locate(self, tile):
        tile = jnp.maximum(tile, 0)
        return self.plan.slot_of(lax.div(tile, self.plan.count)), lax.rem(tile, self.plan.count)

    def edge_row(self, tile, edge):
        slot, local = self.locate(tile)
        at = pl.multiple_of(self.row_base + (2 * local + edge) * self.plan.width, 16)
        return self.held[slot, pl.ds(at, self.plan.width), :]

    def edge_col(self, tile, edge):
        slot, local = self.locate(tile)
        at = pl.multiple_of(self.col_base + (2 * local + edge) * self.plan.rows, 16)
        return self.held[slot, pl.ds(at, self.plan.rows), :]


def held_scratch(plan, part):
    rows = plan.col_base - plan.row_base if part == "rows" else plan.buf_rows - plan.col_base + plan.stat_rows
    return pltpu.VMEM((plan.slots, rows, plan.channels) if plan.direct else (1, 16, plan.channels), bf16)


def buffer_inputs(plan, refs):
    inputs = plan.slots if plan.direct else 1
    return refs[:inputs], refs[inputs:]


def route_kernel(plan, links_ref, *refs):
    bufs, refs = buffer_inputs(plan, refs)
    send_refs, held = refs[:-1], Held(plan, bufs, refs[-1], "rows")
    for k in range(plan.parts):
        first = plan.target(k) * plan.count
        for tile in range(plan.count):
            for edge in range(2):
                at = (2 * tile + edge) * plan.width
                wanted = links_ref[edge, first + tile]
                send_refs[k][at : at + plan.width, :] = held.edge_row(wanted, 1 - edge)


def image_norms(plan, rows_ref, image_ref, held):
    count, channels = plan.count, plan.channels
    group_width = channels // G
    first = lax.axis_index(AXIS) * count
    partial = []
    for slot in range(plan.slots):
        raw = held[slot, 0 : plan.stat_rows, :].astype(f32)
        span = 2 * count
        partial.append(raw[0:span] + raw[span : 2 * span] + raw[2 * span : 3 * span])
    means, inverses = [], []
    for tile in range(count):
        image = image_ref[first + tile]
        weights, pixels = [], []
        area = jnp.int32(0)
        for slot in range(plan.slots):
            base = plan.device_of(slot) * count
            for other in range(count):
                same = image_ref[base + other] == image
                weights.append(jnp.where(same, 1.0, 0.0).astype(f32))
                amount = rows_ref[base + other] * plan.cols
                pixels.append(jnp.maximum(amount, 1).astype(f32))
                area = area + jnp.where(same, amount, 0)
        total = jnp.zeros((1, channels), f32)
        for slot in range(plan.slots):
            for other in range(count):
                total = total + weights[slot * count + other] * partial[slot][other : other + 1]
        amount = jnp.maximum(area * group_width, 1).astype(f32)
        mean = group_total(jnp.broadcast_to(total, (8, channels)), group_width)[0:1] / amount
        total = jnp.zeros((1, channels), f32)
        for slot in range(plan.slots):
            for other in range(count):
                place = slot * count + other
                apart = partial[slot][other : other + 1] / pixels[place] - mean
                spread = partial[slot][count + other : count + other + 1] + pixels[place] * apart * apart
                total = total + weights[place] * spread
        variance = group_total(jnp.broadcast_to(total, (8, channels)), group_width)[0:1] / amount
        means.append(mean)
        inverses.append(lax.rsqrt(variance + epsilon))
    return means, inverses


def halves(mean, inverse, gain_ref, shift_ref):
    scale = inverse * (gain_ref[...] * 0.5)
    shift = shift_ref[...] * 0.5

    def activate(values):
        half = (values.astype(f32) - mean) * scale + shift
        return half + half * jnp.tanh(half)

    return activate


def taps(act, before, after):
    cols = act.shape[0]
    pixel = lax.broadcasted_iota(jnp.int32, act.shape, 0)
    back = jnp.where(pixel == 0, before, pltpu.roll(act, 1, axis=0))
    ahead = jnp.where(pixel == cols - 1, after, pltpu.roll(act, cols - 1, axis=0))
    return [values.astype(bf16) for values in (back, act, ahead)]


def middle_kernel(plan, last, links_ref, rows_ref, image_ref, *refs):
    bufs, refs = buffer_inputs(plan, refs)
    x_ref, gain_ref, shift_ref, offset_ref, weight_ref = refs[:5]
    refs = refs[5:]
    ends_ref = residual_ref = None
    if last:
        (ends_ref, residual_ref), refs = refs[:2], refs[2:]
    if last:
        out_ref, partial_ref, norm_ref, side_ref, rest_ref, held_ref, wide, tiles_ref, sems = refs
    else:
        tiles_ref, partial_ref, norm_ref, side_ref, held_ref, wide = refs
    count, rows, cols, channels = plan.count, plan.rows, plan.cols, plan.channels
    held = Held(plan, bufs, held_ref, "rest")
    means, inverses = image_norms(plan, rows_ref, image_ref, held.held)
    first = lax.axis_index(AXIS) * count
    own_rows = own_values(plan, rows_ref)
    offset = offset_ref[...]
    norm_ref[0 : 2 * count, :] = jnp.concatenate(means + inverses, axis=0)
    copies = []
    for tile in range(count):
        valid = own_rows[tile]
        link = [links_ref[column, first + tile] for column in range(4)]
        activate = halves(means[tile], inverses[tile], gain_ref, shift_ref)
        left = jnp.where(link[2] >= 0, activate(held.edge_col(link[2], 1)), 0.0)
        right = jnp.where(link[3] >= 0, activate(held.edge_col(link[3], 0)), 0.0)
        corners = []
        for place in range(4):
            beside = links_ref[2 + place % 2, jnp.maximum(link[place // 2], 0)]
            beside = jnp.where(link[place // 2] >= 0, beside, -1)
            row = 0 if place // 2 else rows - 1
            corner = activate(held.edge_col(beside, 1 - place % 2))[row : row + 1]
            corners.append(jnp.where(beside >= 0, corner, 0.0))
        side_ref[8 * tile : 8 * tile + 4, :] = jnp.concatenate(corners, axis=0)

        depth = 3 * channels
        nothing = jnp.zeros((cols, depth), bf16)
        wide[tile, 0, :, 0:depth] = nothing
        wide[tile, rows // 2, :, depth : 2 * depth] = nothing
        for row in range(rows):
            if ends_ref is not None and row in (0, rows - 1):
                source = ends_ref[2 * tile + (row > 0)]
            else:
                source = x_ref[tile, row]
            act = jnp.where(row < valid, activate(source), 0.0)
            before = jnp.where(row < valid, left[row : row + 1], 0.0)
            after = jnp.where(row < valid, right[row : row + 1], 0.0)
            lane = ((row + 1) % 2) * depth
            for tap, values in enumerate(taps(act, before, after)):
                at = lane + tap * channels
                wide[tile, (row + 1) // 2, :, at : at + channels] = values

        pairs = rows // 2
        step = 1
        gathered = None
        for pair in range(0, pairs, step):
            upper = wide[tile, pair : pair + step].reshape(step * cols, 2 * depth)
            lower = wide[tile, pair + 1 : pair + step + 1].reshape(step * cols, 2 * depth)
            window = jnp.concatenate([upper, lower], axis=1)
            summed = jnp.dot(window, weight_ref[...], preferred_element_type=f32)
            inner = {}
            for row in range(2 * pair, 2 * (pair + step)):
                at, lane = (row // 2 - pair) * cols, (row % 2) * channels
                part = summed[at : at + cols, lane : lane + channels] + offset
                if last:
                    part = part + residual_ref[tile, row].astype(f32)
                if row in (0, rows - 1):
                    partial_ref[2 * tile + (row > 0)] = part
                    continue
                part = jnp.where(row < valid, part, 0.0).astype(bf16)
                if last and tile == count - 1:
                    rest_ref[row - 1] = part
                    continue
                tiles_ref[tile, row] = part
                inner[row] = part.astype(f32)
            if last:
                if not inner:
                    continue
                band = pl.ds(min(inner), len(inner))
                sem = sems.at[tile * pairs + pair]
                copy = pltpu.make_async_copy(tiles_ref.at[tile, band], out_ref.at[tile, band], sem)
                copy.start()
                copies.append(copy)
            else:
                found = column_sums(lambda row: inner[row], sorted(inner), valid)
                gathered = found if gathered is None else merge_sums(gathered, found)
        if not last:
            norm_ref[(2 * count + tile) : (2 * count + tile) + 1, :] = gathered[1]
            norm_ref[(3 * count + tile) : (3 * count + tile) + 1, :] = gathered[2]
            for side, column in enumerate((0, cols - 1)):
                picked = [tiles_ref[tile, row, column : column + 1, :].astype(f32) for row in range(1, rows - 1)]
                at = 8 * count + (2 * tile + side) * rows
                side_ref[at + 1 : at + rows - 1, :] = jnp.concatenate(picked, axis=0)
    for copy in copies:
        copy.wait()


def ends_kernel(plan, last, links_ref, rows_ref, *refs):
    halo_refs, refs = refs[: plan.parts], refs[plan.parts :]
    partial_ref, norm_ref, side_ref, gain_ref, shift_ref, weight_ref = refs[:6]
    refs = refs[6:]
    count, rows, cols, channels = plan.count, plan.rows, plan.cols, plan.channels
    if last:
        rest_ref, _, out_ref, halo, ends_ref, sems = refs
    else:
        ends_ref, buf_refs, halo = refs[0], refs[1:-1], refs[-1]
    first = lax.axis_index(AXIS) * count
    own_rows = own_values(plan, rows_ref)
    for k in range(plan.parts):
        for place in range(2 * count):
            at = place * plan.width
            halo[place, plan.window(k), :] = halo_refs[k][at : at + plan.width, :]
    depth = 3 * channels
    copies, sums, spreads, columns = [], [], [], []
    if last:
        target = out_ref.at[count - 1, pl.ds(1, rows - 2)]
        copies.append(pltpu.make_async_copy(rest_ref, target, sems.at[2 * count]))
        copies[-1].start()
    for tile in range(count):
        valid = own_rows[tile]
        activate = halves(
            norm_ref[tile : tile + 1, :], norm_ref[count + tile : count + tile + 1, :], gain_ref, shift_ref
        )
        values = []
        for edge, row in enumerate((0, rows - 1)):
            place = 2 * tile + edge
            present = links_ref[edge, first + tile] >= 0
            act = jnp.where(present, activate(halo[place]), 0.0)
            at = 8 * tile + 2 * edge
            wide = jnp.concatenate(taps(act, side_ref[at : at + 1, :], side_ref[at + 1 : at + 2, :]), axis=1)
            weight = weight_ref[3 * edge * depth : (3 * edge + 1) * depth, edge * channels : (edge + 1) * channels]
            part = partial_ref[place] + jnp.dot(wide, weight, preferred_element_type=f32)
            result = jnp.where(row < valid, part, 0.0).astype(bf16)
            ends_ref[place] = result
            values.append(result.astype(f32))
            if last:
                copies.append(pltpu.make_async_copy(ends_ref.at[place], out_ref.at[tile, row], sems.at[place]))
                copies[-1].start()
        if last:
            continue
        found = column_sums(lambda row: values[row > 0], (0, rows - 1), valid)
        inner = (
            jnp.maximum((jnp.minimum(valid, rows - 1) - 1) * cols, 0).astype(f32),
            norm_ref[2 * count + tile : 2 * count + tile + 1, :],
            norm_ref[3 * count + tile : 3 * count + tile + 1, :],
        )
        _, total, spread = merge_sums(inner, found)
        sums.append(total)
        spreads.append(spread)
        line = lax.broadcasted_iota(jnp.int32, (rows, channels), 0)
        for side, column in enumerate((0, cols - 1)):
            at = 8 * count + (2 * tile + side) * rows
            picked = side_ref[at : at + rows, :]
            picked = jnp.where(line == 0, values[0][column : column + 1], picked)
            picked = jnp.where(line == rows - 1, values[1][column : column + 1], picked)
            columns.append(picked.astype(bf16))
    if not last:

        def edge_of(tile, edge, window):
            return ends_ref[2 * tile + edge, window, :]

        fill_buffers(plan, pack_stats(plan, sums, spreads), edge_of, columns, buf_refs)
    for copy in copies:
        copy.wait()


def paired_weights(kernel):
    upper = jnp.pad(kernel, ((0, 1), (0, 0), (0, 0), (0, 0)))
    lower = jnp.pad(kernel, ((1, 0), (0, 0), (0, 0), (0, 0)))
    both = jnp.concatenate([upper, lower], axis=-1)
    return both.reshape(-1, both.shape[-1])


def shards(
    feature_tiles,
    neighbours,
    valid_rows,
    tile_image,
    gain_one,
    shift_one,
    kernel_one,
    offset_one,
    gain_two,
    shift_two,
    kernel_two,
    offset_two,
    *,
    size,
):
    count, rows, cols, channels = feature_tiles.shape
    plan = Plan(size, count, rows, cols, channels)
    buf_shape = [jax.ShapeDtypeStruct((plan.buf_rows, channels), bf16)] * plan.targets
    limit = 24 * 1024 * 1024
    params = pltpu.CompilerParams(vmem_limit_bytes=limit)

    def swap(array, distance):
        return lax.ppermute(array, AXIS, [(i, i ^ distance) for i in range(size)])

    def spread(arrays):
        result = [arrays[0]]
        for k in range(1, len(arrays)):
            result.append(swap(arrays[k], 2 * k))
        return result

    def exchange(bufs):
        if not plan.direct:
            return [lax.all_gather(bufs[0], AXIS)]
        own = spread(bufs)
        return own + [swap(array, 1) for array in own]

    def shape(dims, dtype=f32):
        return jax.ShapeDtypeStruct(dims, dtype)

    partial_shape = shape((2 * count, cols, channels))
    norm_shape = shape((round_up(4 * count, 8), channels))
    side_shape = shape((8 * count + 2 * count * rows, channels))
    ends_shape = shape((2 * count, cols, channels), bf16)
    tiles_shape = shape(feature_tiles.shape, bf16)

    def stage(last, source, ends, bufs, gain, shift, kernel, offset):
        arrays = exchange(bufs)
        send = pl.pallas_call(
            functools.partial(route_kernel, plan),
            out_shape=[shape((2 * count * plan.width, channels), bf16)] * plan.parts,
            in_specs=[SMEM] + [VMEM] * len(arrays),
            out_specs=[VMEM] * plan.parts,
            scratch_shapes=[held_scratch(plan, "rows")],
            compiler_params=params,
        )(scalars[0], *arrays)
        halo = spread(send)
        weights = paired_weights(kernel)
        gain, shift, offset = gain[None], shift[None], offset[None]
        operands = arrays + [source, gain, shift, offset, weights] + ([ends, features] if last else [])
        flops = 2 * count * rows * cols * 9 * channels * channels
        tiles, partial, norm, side, *rest = pl.pallas_call(
            functools.partial(middle_kernel, plan, last),
            out_shape=[tiles_shape, partial_shape, norm_shape, side_shape] + [shape((rows - 2, cols, channels), bf16)] * last,
            in_specs=[SMEM] * 3 + [VMEM] * len(operands),
            out_specs=[HBM if last else VMEM] + [VMEM] * (3 + last),
            scratch_shapes=[held_scratch(plan, "rest"), pltpu.VMEM((count, rows // 2 + 1, cols, 6 * channels), bf16)]
            + ([pltpu.VMEM(feature_tiles.shape, bf16), pltpu.SemaphoreType.DMA((count * rows // 2,))] if last else []),
            compiler_params=params,
            cost_estimate=pl.CostEstimate(flops=flops, bytes_accessed=4 * feature_tiles.size, transcendentals=0),
        )(*scalars, *operands)
        operands = halo + [partial, norm, side, gain, shift, weights] + rest
        scratch = [pltpu.VMEM((2 * count, cols, channels), bf16)]
        if last:
            return pl.pallas_call(
                functools.partial(ends_kernel, plan, last),
                out_shape=tiles_shape,
                in_specs=[SMEM] * 2 + [VMEM] * len(operands) + [HBM],
                out_specs=HBM,
                input_output_aliases={2 + len(operands): 0},
                scratch_shapes=scratch + scratch + [pltpu.SemaphoreType.DMA((2 * count + 1,))],
                compiler_params=params,
            )(*scalars[:2], *operands, tiles)
        ends, *bufs = pl.pallas_call(
            functools.partial(ends_kernel, plan, last),
            out_shape=[ends_shape] + buf_shape,
            in_specs=[SMEM] * 2 + [VMEM] * len(operands),
            out_specs=[VMEM] * (1 + plan.targets),
            scratch_shapes=scratch,
            compiler_params=params,
        )(*scalars[:2], *operands)
        return tiles, ends, bufs

    tables = (neighbours.T, valid_rows, tile_image)
    inputs = [pltpu.with_memory_space_constraint(array, pltpu.HBM) for array in (*tables, feature_tiles)]
    found = pl.pallas_call(
        functools.partial(edges_kernel, plan),
        out_shape=[pltpu.SMEM(table.shape, jnp.int32) for table in tables] + [tiles_shape] + buf_shape,
        in_specs=[HBM] * 4,
        out_specs=[SMEM] * 3 + [VMEM] * (1 + plan.targets),
        scratch_shapes=[pltpu.SemaphoreType.DMA((3 + 4 * count,))],
        compiler_params=params,
        name="edges",
    )(*inputs)
    scalars, features, bufs = found[:3], found[3], found[4:]
    hidden, ends, bufs = stage(False, features, None, bufs, gain_one, shift_one, kernel_one, offset_one)
    return stage(True, hidden, ends, bufs, gain_two, shift_two, kernel_two, offset_two)


def solution(mesh):
    in_specs = (
        P(("rep", "tile"), None, None, None),
        P("rep", None),
        P("rep"),
        P("rep"),
        P(),
        P(),
        P(),
        P(),
        P(),
        P(),
        P(),
        P(),
    )
    out_specs = P(("rep", "tile"), None, None, None)

    def body(*args):
        return shards(*args, size=mesh.shape[AXIS])

    return jax.shard_map(body, mesh=mesh, in_specs=in_specs, out_specs=out_specs, check_vma=False)
```

```python
import functools

import jax
import jax.numpy as jnp
from jax import lax
from jax.experimental import pallas as pl
from jax.experimental.pallas import tpu as pltpu
from jax.sharding import PartitionSpec as P


G = 32
AXIS = "tile"
epsilon = 1e-06
f32 = jnp.float32
bf16 = jnp.bfloat16


VMEM = pl.BlockSpec(memory_space=pltpu.VMEM)
SMEM = pl.BlockSpec(memory_space=pltpu.SMEM)
HBM = pl.BlockSpec(memory_space=pltpu.HBM)


def round_up(value, step):
    return -(-value // step) * step


class Plan:
    def __init__(self, size, count, rows, cols, channels):
        self.size, self.count, self.rows, self.cols, self.channels = size, count, rows, cols, channels
        chips = size // 2
        self.direct = size % 2 == 0 and chips in (2, 4, 8) and cols % 32 == 0
        self.targets = chips if self.direct else 1
        self.parts = 2 if self.direct else 1
        self.width = cols // self.parts
        self.stat_rows = round_up(6 * count, 16)
        self.row_base = self.stat_rows
        self.col_base = self.row_base + 2 * count * self.width
        self.buf_rows = self.col_base + 2 * count * rows
        self.slots = size

    def place(self):
        index = lax.axis_index(AXIS)
        return lax.div(index, 2), lax.rem(index, 2)

    def window(self, k):
        if not self.direct:
            return pl.ds(0, self.width)
        part = lax.bitwise_and(lax.bitwise_xor(self.place()[0], k), 1)
        return pl.ds(pl.multiple_of(part * self.width, 16), self.width)

    def slot_of(self, device):
        if not self.direct:
            return device
        chip, core = self.place()
        other = lax.bitwise_xor(lax.rem(device, 2), core)
        return other * self.targets + lax.bitwise_xor(lax.div(device, 2), chip)

    def device_of(self, slot):
        if not self.direct:
            return slot
        chip, core = self.place()
        return lax.bitwise_xor(chip, slot % self.targets) * 2 + lax.bitwise_xor(core, slot // self.targets)

    def target(self, k):
        if not self.direct:
            return lax.axis_index(AXIS)
        chip, core = self.place()
        return lax.bitwise_xor(chip, k) * 2 + core


def split_three(values):
    high = values.astype(bf16)
    rest = values - high.astype(f32)
    middle = rest.astype(bf16)
    low = (rest - middle.astype(f32)).astype(bf16)
    return high.astype(f32), middle.astype(f32), low.astype(f32)


def fold_rows(values):
    return values.reshape(-1, 8, values.shape[-1]).sum(axis=0)


def mean_of(values):
    return jnp.sum(fold_rows(values), axis=0, keepdims=True) * (1.0 / values.shape[0])


def row_sums(values_of, rows, pivot):
    found = []
    for row in rows:
        apart = values_of(row) - pivot
        found.append((row, fold_rows(apart), fold_rows(apart * apart)))
    return found


def masked_sums(width, pivot, found, valid):
    pixels = jnp.int32(0)
    total = spread = None
    for row, part, square in found:
        inside = row < valid
        pixels = pixels + jnp.where(inside, width, 0)
        part, square = jnp.where(inside, part, 0.0), jnp.where(inside, square, 0.0)
        total = part if total is None else total + part
        spread = square if spread is None else spread + square
    total = jnp.sum(total, axis=0, keepdims=True)
    spread = jnp.sum(spread, axis=0, keepdims=True)
    pixels = pixels.astype(f32)
    spread = jnp.maximum(spread - total * (total / jnp.maximum(pixels, 1.0)), 0.0)
    return pixels, total + pixels * pivot, spread


def column_sums(values_of, rows, valid):
    rows = list(rows)
    first = values_of(rows[0])
    pivot = mean_of(first)
    return masked_sums(first.shape[0], pivot, row_sums(values_of, rows, pivot), valid)


def merge_sums(one, two):
    pixels, other = jnp.maximum(one[0], 1.0), jnp.maximum(two[0], 1.0)
    apart = one[1] / pixels - two[1] / other
    weight = jnp.where(jnp.minimum(one[0], two[0]) > 0, pixels * other / (pixels + other), 0.0)
    return one[0] + two[0], one[1] + two[1], one[2] + two[2] + apart * apart * weight


def pack_stats(plan, sums, spreads):
    parts = list(split_three(jnp.concatenate(sums + spreads, axis=0)))
    padding = plan.stat_rows - 6 * plan.count
    if padding:
        parts.append(jnp.zeros((padding, plan.channels), f32))
    return jnp.concatenate(parts, axis=0).astype(bf16)


def fill_buffers(plan, stats, edge_of, columns, buf_refs):
    for k in range(plan.targets):
        buf_refs[k][0 : plan.stat_rows, :] = stats
        window = plan.window(k)
        for tile in range(plan.count):
            for edge in range(2):
                at = plan.row_base + (2 * tile + edge) * plan.width
                buf_refs[k][at : at + plan.width, :] = edge_of(tile, edge, window)
        for place, column in enumerate(columns):
            at = plan.col_base + place * plan.rows
            buf_refs[k][at : at + plan.rows, :] = column


def own_values(plan, ref):
    first = lax.axis_index(AXIS) * plan.count
    return [ref[first + tile] for tile in range(plan.count)]


def edges_kernel(plan, links_hbm, rows_hbm, image_hbm, x_hbm, links_ref, rows_ref, image_ref, *refs):
    x_ref, buf_refs, sems = refs[0], refs[1:-1], refs[-1]
    tables = [
        pltpu.make_async_copy(source, target, sems.at[place])
        for place, (source, target) in enumerate(
            ((rows_hbm, rows_ref), (links_hbm, links_ref), (image_hbm, image_ref))
        )
    ]
    bands = 4
    height = plan.rows // bands
    copies = {}
    for tile in range(plan.count):
        for band in range(bands):
            window = pl.ds(band * height, height)
            sem = sems.at[3 + tile * bands + band]
            copies[tile, band] = pltpu.make_async_copy(x_hbm.at[tile, window], x_ref.at[tile, window], sem)
    for copy in [tables[0], *copies.values(), *tables[1:]]:
        copy.start()
    found, columns = [], []
    for tile in range(plan.count):
        pieces = []
        for band in range(bands):
            copies[tile, band].wait()
            rows = range(band * height, (band + 1) * height)
            if band == 0:
                pivot = mean_of(x_ref[tile, 0].astype(f32))
            pieces += row_sums(lambda row: x_ref[tile, row].astype(f32), rows, pivot)
        found.append((plan.cols, pivot, pieces))
        for column in (0, plan.cols - 1):
            picked = [x_ref[tile, row, column : column + 1, :].astype(f32) for row in range(plan.rows)]
            columns.append(jnp.concatenate(picked, axis=0).astype(bf16))
    tables[0].wait()
    own_rows = own_values(plan, rows_ref)
    sums, spreads = [], []
    for tile in range(plan.count):
        _, total, spread = masked_sums(*found[tile], own_rows[tile])
        sums.append(total)
        spreads.append(spread)

    def edge_of(tile, edge, window):
        return x_ref[tile, edge * (plan.rows - 1), window, :]

    fill_buffers(plan, pack_stats(plan, sums, spreads), edge_of, columns, buf_refs)
    for copy in tables[1:]:
        copy.wait()


def group_total(values, group_width):
    lanes = values.shape[-1]
    lane = lax.broadcasted_iota(jnp.int32, values.shape, 1)
    step = 1
    while step < group_width:
        ahead = pltpu.roll(values, lanes - step, axis=1)
        behind = pltpu.roll(values, step, axis=1)
        values = values + jnp.where(lax.bitwise_and(lane, step) == 0, ahead, behind)
        step *= 2
    return values


class Held:
    def __init__(self, plan, bufs, held, part):
        self.plan = plan
        self.row_base, self.col_base = plan.row_base, plan.col_base
        self.held = bufs[0]
        if plan.direct:
            self.held = held
            self.row_base, self.col_base = 0, plan.stat_rows
            for slot in range(plan.slots):
                if part == "rows":
                    held[slot] = bufs[slot][plan.row_base : plan.col_base, :]
                else:
                    held[slot, 0 : plan.stat_rows, :] = bufs[slot][0 : plan.stat_rows, :]
                    held[slot, plan.stat_rows :, :] = bufs[slot][plan.col_base :, :]

    def locate(self, tile):
        tile = jnp.maximum(tile, 0)
        return self.plan.slot_of(lax.div(tile, self.plan.count)), lax.rem(tile, self.plan.count)

    def edge_row(self, tile, edge):
        slot, local = self.locate(tile)
        at = pl.multiple_of(self.row_base + (2 * local + edge) * self.plan.width, 16)
        return self.held[slot, pl.ds(at, self.plan.width), :]

    def edge_col(self, tile, edge):
        slot, local = self.locate(tile)
        at = pl.multiple_of(self.col_base + (2 * local + edge) * self.plan.rows, 16)
        return self.held[slot, pl.ds(at, self.plan.rows), :]


def held_scratch(plan, part):
    rows = plan.col_base - plan.row_base if part == "rows" else plan.buf_rows - plan.col_base + plan.stat_rows
    return pltpu.VMEM((plan.slots, rows, plan.channels) if plan.direct else (1, 16, plan.channels), bf16)


def buffer_inputs(plan, refs):
    inputs = plan.slots if plan.direct else 1
    return refs[:inputs], refs[inputs:]


def route_kernel(plan, links_ref, *refs):
    bufs, refs = buffer_inputs(plan, refs)
    send_refs, held = refs[:-1], Held(plan, bufs, refs[-1], "rows")
    for k in range(plan.parts):
        first = plan.target(k) * plan.count
        for tile in range(plan.count):
            for edge in range(2):
                at = (2 * tile + edge) * plan.width
                wanted = links_ref[edge, first + tile]
                send_refs[k][at : at + plan.width, :] = held.edge_row(wanted, 1 - edge)


def image_norms(plan, rows_ref, image_ref, held):
    count, channels = plan.count, plan.channels
    group_width = channels // G
    first = lax.axis_index(AXIS) * count
    partial = []
    for slot in range(plan.slots):
        raw = held[slot, 0 : plan.stat_rows, :].astype(f32)
        span = 2 * count
        partial.append(raw[0:span] + raw[span : 2 * span] + raw[2 * span : 3 * span])
    means, inverses = [], []
    for tile in range(count):
        image = image_ref[first + tile]
        weights, pixels = [], []
        area = jnp.int32(0)
        for slot in range(plan.slots):
            base = plan.device_of(slot) * count
            for other in range(count):
                same = image_ref[base + other] == image
                weights.append(jnp.where(same, 1.0, 0.0).astype(f32))
                amount = rows_ref[base + other] * plan.cols
                pixels.append(jnp.maximum(amount, 1).astype(f32))
                area = area + jnp.where(same, amount, 0)
        total = jnp.zeros((1, channels), f32)
        for slot in range(plan.slots):
            for other in range(count):
                total = total + weights[slot * count + other] * partial[slot][other : other + 1]
        amount = jnp.maximum(area * group_width, 1).astype(f32)
        mean = group_total(jnp.broadcast_to(total, (8, channels)), group_width)[0:1] / amount
        total = jnp.zeros((1, channels), f32)
        for slot in range(plan.slots):
            for other in range(count):
                place = slot * count + other
                apart = partial[slot][other : other + 1] / pixels[place] - mean
                spread = partial[slot][count + other : count + other + 1] + pixels[place] * apart * apart
                total = total + weights[place] * spread
        variance = group_total(jnp.broadcast_to(total, (8, channels)), group_width)[0:1] / amount
        means.append(mean)
        inverses.append(lax.rsqrt(variance + epsilon))
    return means, inverses


def halves(mean, inverse, gain_ref, shift_ref):
    scale = inverse * (gain_ref[...] * 0.5)
    shift = shift_ref[...] * 0.5

    def activate(values):
        half = (values.astype(f32) - mean) * scale + shift
        return half + half * jnp.tanh(half)

    return activate


def taps(act, before, after):
    cols = act.shape[0]
    pixel = lax.broadcasted_iota(jnp.int32, act.shape, 0)
    back = jnp.where(pixel == 0, before, pltpu.roll(act, 1, axis=0))
    ahead = jnp.where(pixel == cols - 1, after, pltpu.roll(act, cols - 1, axis=0))
    return [values.astype(bf16) for values in (back, act, ahead)]


def middle_kernel(plan, last, links_ref, rows_ref, image_ref, *refs):
    bufs, refs = buffer_inputs(plan, refs)
    x_ref, gain_ref, shift_ref, offset_ref, weight_ref = refs[:5]
    refs = refs[5:]
    ends_ref = residual_ref = None
    if last:
        (ends_ref, residual_ref), refs = refs[:2], refs[2:]
    if last:
        out_ref, partial_ref, norm_ref, side_ref, rest_ref, held_ref, wide, tiles_ref, sems = refs
    else:
        tiles_ref, partial_ref, norm_ref, side_ref, held_ref, wide = refs
    count, rows, cols, channels = plan.count, plan.rows, plan.cols, plan.channels
    held = Held(plan, bufs, held_ref, "rest")
    means, inverses = image_norms(plan, rows_ref, image_ref, held.held)
    first = lax.axis_index(AXIS) * count
    own_rows = own_values(plan, rows_ref)
    offset = offset_ref[...]
    norm_ref[0 : 2 * count, :] = jnp.concatenate(means + inverses, axis=0)
    copies = []
    for tile in range(count):
        valid = own_rows[tile]
        link = [links_ref[column, first + tile] for column in range(4)]
        activate = halves(means[tile], inverses[tile], gain_ref, shift_ref)
        left = jnp.where(link[2] >= 0, activate(held.edge_col(link[2], 1)), 0.0)
        right = jnp.where(link[3] >= 0, activate(held.edge_col(link[3], 0)), 0.0)
        corners = []
        for place in range(4):
            beside = links_ref[2 + place % 2, jnp.maximum(link[place // 2], 0)]
            beside = jnp.where(link[place // 2] >= 0, beside, -1)
            row = 0 if place // 2 else rows - 1
            corner = activate(held.edge_col(beside, 1 - place % 2))[row : row + 1]
            corners.append(jnp.where(beside >= 0, corner, 0.0))
        side_ref[8 * tile : 8 * tile + 4, :] = jnp.concatenate(corners, axis=0)

        depth = 3 * channels
        nothing = jnp.zeros((cols, depth), bf16)
        wide[tile, 0, :, 0:depth] = nothing
        wide[tile, rows // 2, :, depth : 2 * depth] = nothing
        for row in range(rows):
            if ends_ref is not None and row in (0, rows - 1):
                source = ends_ref[2 * tile + (row > 0)]
            else:
                source = x_ref[tile, row]
            act = jnp.where(row < valid, activate(source), 0.0)
            before = jnp.where(row < valid, left[row : row + 1], 0.0)
            after = jnp.where(row < valid, right[row : row + 1], 0.0)
            lane = ((row + 1) % 2) * depth
            for tap, values in enumerate(taps(act, before, after)):
                at = lane + tap * channels
                wide[tile, (row + 1) // 2, :, at : at + channels] = values

        pairs = rows // 2
        step = 1
        gathered = None
        for pair in range(0, pairs, step):
            upper = wide[tile, pair : pair + step].reshape(step * cols, 2 * depth)
            lower = wide[tile, pair + 1 : pair + step + 1].reshape(step * cols, 2 * depth)
            window = jnp.concatenate([upper, lower], axis=1)
            summed = jnp.dot(window, weight_ref[...], preferred_element_type=f32)
            inner = {}
            for row in range(2 * pair, 2 * (pair + step)):
                at, lane = (row // 2 - pair) * cols, (row % 2) * channels
                part = summed[at : at + cols, lane : lane + channels] + offset
                if last:
                    part = part + residual_ref[tile, row].astype(f32)
                if row in (0, rows - 1):
                    partial_ref[2 * tile + (row > 0)] = part
                    continue
                part = jnp.where(row < valid, part, 0.0).astype(bf16)
                if last and tile == count - 1:
                    rest_ref[row - 1] = part
                    continue
                tiles_ref[tile, row] = part
                inner[row] = part.astype(f32)
            if last:
                if not inner:
                    continue
                band = pl.ds(min(inner), len(inner))
                sem = sems.at[tile * pairs + pair]
                copy = pltpu.make_async_copy(tiles_ref.at[tile, band], out_ref.at[tile, band], sem)
                copy.start()
                copies.append(copy)
            else:
                found = column_sums(lambda row: inner[row], sorted(inner), valid)
                gathered = found if gathered is None else merge_sums(gathered, found)
        if not last:
            norm_ref[(2 * count + tile) : (2 * count + tile) + 1, :] = gathered[1]
            norm_ref[(3 * count + tile) : (3 * count + tile) + 1, :] = gathered[2]
            for side, column in enumerate((0, cols - 1)):
                picked = [tiles_ref[tile, row, column : column + 1, :].astype(f32) for row in range(1, rows - 1)]
                at = 8 * count + (2 * tile + side) * rows
                side_ref[at + 1 : at + rows - 1, :] = jnp.concatenate(picked, axis=0)
    for copy in copies:
        copy.wait()


def ends_kernel(plan, last, links_ref, rows_ref, *refs):
    halo_refs, refs = refs[: plan.parts], refs[plan.parts :]
    partial_ref, norm_ref, side_ref, gain_ref, shift_ref, weight_ref = refs[:6]
    refs = refs[6:]
    count, rows, cols, channels = plan.count, plan.rows, plan.cols, plan.channels
    if last:
        rest_ref, _, out_ref, halo, ends_ref, sems = refs
    else:
        ends_ref, buf_refs, halo = refs[0], refs[1:-1], refs[-1]
    first = lax.axis_index(AXIS) * count
    own_rows = own_values(plan, rows_ref)
    for k in range(plan.parts):
        for place in range(2 * count):
            at = place * plan.width
            halo[place, plan.window(k), :] = halo_refs[k][at : at + plan.width, :]
    depth = 3 * channels
    copies, sums, spreads, columns = [], [], [], []
    if last:
        target = out_ref.at[count - 1, pl.ds(1, rows - 2)]
        copies.append(pltpu.make_async_copy(rest_ref, target, sems.at[2 * count]))
        copies[-1].start()
    for tile in range(count):
        valid = own_rows[tile]
        activate = halves(
            norm_ref[tile : tile + 1, :], norm_ref[count + tile : count + tile + 1, :], gain_ref, shift_ref
        )
        values = []
        for edge, row in enumerate((0, rows - 1)):
            place = 2 * tile + edge
            present = links_ref[edge, first + tile] >= 0
            act = jnp.where(present, activate(halo[place]), 0.0)
            at = 8 * tile + 2 * edge
            wide = jnp.concatenate(taps(act, side_ref[at : at + 1, :], side_ref[at + 1 : at + 2, :]), axis=1)
            weight = weight_ref[3 * edge * depth : (3 * edge + 1) * depth, edge * channels : (edge + 1) * channels]
            part = partial_ref[place] + jnp.dot(wide, weight, preferred_element_type=f32)
            result = jnp.where(row < valid, part, 0.0).astype(bf16)
            ends_ref[place] = result
            values.append(result.astype(f32))
            if last:
                copies.append(pltpu.make_async_copy(ends_ref.at[place], out_ref.at[tile, row], sems.at[place]))
                copies[-1].start()
        if last:
            continue
        found = column_sums(lambda row: values[row > 0], (0, rows - 1), valid)
        inner = (
            jnp.maximum((jnp.minimum(valid, rows - 1) - 1) * cols, 0).astype(f32),
            norm_ref[2 * count + tile : 2 * count + tile + 1, :],
            norm_ref[3 * count + tile : 3 * count + tile + 1, :],
        )
        _, total, spread = merge_sums(inner, found)
        sums.append(total)
        spreads.append(spread)
        line = lax.broadcasted_iota(jnp.int32, (rows, channels), 0)
        for side, column in enumerate((0, cols - 1)):
            at = 8 * count + (2 * tile + side) * rows
            picked = side_ref[at : at + rows, :]
            picked = jnp.where(line == 0, values[0][column : column + 1], picked)
            picked = jnp.where(line == rows - 1, values[1][column : column + 1], picked)
            columns.append(picked.astype(bf16))
    if not last:

        def edge_of(tile, edge, window):
            return ends_ref[2 * tile + edge, window, :]

        fill_buffers(plan, pack_stats(plan, sums, spreads), edge_of, columns, buf_refs)
    for copy in copies:
        copy.wait()


def paired_weights(kernel):
    upper = jnp.pad(kernel, ((0, 1), (0, 0), (0, 0), (0, 0)))
    lower = jnp.pad(kernel, ((1, 0), (0, 0), (0, 0), (0, 0)))
    both = jnp.concatenate([upper, lower], axis=-1)
    return both.reshape(-1, both.shape[-1])


def shards(
    feature_tiles,
    neighbours,
    valid_rows,
    tile_image,
    gain_one,
    shift_one,
    kernel_one,
    offset_one,
    gain_two,
    shift_two,
    kernel_two,
    offset_two,
    *,
    size,
):
    count, rows, cols, channels = feature_tiles.shape
    plan = Plan(size, count, rows, cols, channels)
    buf_shape = [jax.ShapeDtypeStruct((plan.buf_rows, channels), bf16)] * plan.targets
    limit = 24 * 1024 * 1024
    params = pltpu.CompilerParams(vmem_limit_bytes=limit)

    def swap(array, distance):
        return lax.ppermute(array, AXIS, [(i, i ^ distance) for i in range(size)])

    def spread(arrays):
        result = [arrays[0]]
        for k in range(1, len(arrays)):
            result.append(swap(arrays[k], 2 * k))
        return result

    def exchange(bufs):
        if not plan.direct:
            return [lax.all_gather(bufs[0], AXIS)]
        own = spread(bufs)
        other = []
        for array in own:
            other.append(swap(array, 1))
        return own + other

    def shape(dims, dtype=f32):
        return jax.ShapeDtypeStruct(dims, dtype)

    partial_shape = shape((2 * count, cols, channels))
    norm_shape = shape((round_up(4 * count, 8), channels))
    side_shape = shape((8 * count + 2 * count * rows, channels))
    ends_shape = shape((2 * count, cols, channels), bf16)
    tiles_shape = shape(feature_tiles.shape, bf16)

    def stage(last, source, ends, bufs, gain, shift, kernel, offset):
        arrays = exchange(bufs)
        send = pl.pallas_call(
            functools.partial(route_kernel, plan),
            out_shape=[shape((2 * count * plan.width, channels), bf16)] * plan.parts,
            in_specs=[SMEM] + [VMEM] * len(arrays),
            out_specs=[VMEM] * plan.parts,
            scratch_shapes=[held_scratch(plan, "rows")],
            compiler_params=params,
        )(scalars[0], *arrays)
        halo = spread(send)
        weights = paired_weights(kernel)
        gain, shift, offset = gain[None], shift[None], offset[None]
        operands = arrays + [source, gain, shift, offset, weights] + ([ends, features] if last else [])
        flops = 2 * count * rows * cols * 9 * channels * channels
        tiles, partial, norm, side, *rest = pl.pallas_call(
            functools.partial(middle_kernel, plan, last),
            out_shape=[tiles_shape, partial_shape, norm_shape, side_shape] + [shape((rows - 2, cols, channels), bf16)] * last,
            in_specs=[SMEM] * 3 + [VMEM] * len(operands),
            out_specs=[HBM if last else VMEM] + [VMEM] * (3 + last),
            scratch_shapes=[held_scratch(plan, "rest"), pltpu.VMEM((count, rows // 2 + 1, cols, 6 * channels), bf16)]
            + ([pltpu.VMEM(feature_tiles.shape, bf16), pltpu.SemaphoreType.DMA((count * rows // 2,))] if last else []),
            compiler_params=params,
            cost_estimate=pl.CostEstimate(flops=flops, bytes_accessed=4 * feature_tiles.size, transcendentals=0),
        )(*scalars, *operands)
        operands = halo + [partial, norm, side, gain, shift, weights] + rest
        scratch = [pltpu.VMEM((2 * count, cols, channels), bf16)]
        if last:
            return pl.pallas_call(
                functools.partial(ends_kernel, plan, last),
                out_shape=tiles_shape,
                in_specs=[SMEM] * 2 + [VMEM] * len(operands) + [HBM],
                out_specs=HBM,
                input_output_aliases={2 + len(operands): 0},
                scratch_shapes=scratch + scratch + [pltpu.SemaphoreType.DMA((2 * count + 1,))],
                compiler_params=params,
            )(*scalars[:2], *operands, tiles)
        ends, *bufs = pl.pallas_call(
            functools.partial(ends_kernel, plan, last),
            out_shape=[ends_shape] + buf_shape,
            in_specs=[SMEM] * 2 + [VMEM] * len(operands),
            out_specs=[VMEM] * (1 + plan.targets),
            scratch_shapes=scratch,
            compiler_params=params,
        )(*scalars[:2], *operands)
        return tiles, ends, bufs

    tables = (neighbours.T, valid_rows, tile_image)
    inputs = [pltpu.with_memory_space_constraint(array, pltpu.HBM) for array in (*tables, feature_tiles)]
    found = pl.pallas_call(
        functools.partial(edges_kernel, plan),
        out_shape=[pltpu.SMEM(table.shape, jnp.int32) for table in tables] + [tiles_shape] + buf_shape,
        in_specs=[HBM] * 4,
        out_specs=[SMEM] * 3 + [VMEM] * (1 + plan.targets),
        scratch_shapes=[pltpu.SemaphoreType.DMA((3 + 4 * count,))],
        compiler_params=params,
        name="edges",
    )(*inputs)
    scalars, features, bufs = found[:3], found[3], found[4:]
    hidden, ends, bufs = stage(False, features, None, bufs, gain_one, shift_one, kernel_one, offset_one)
    return stage(True, hidden, ends, bufs, gain_two, shift_two, kernel_two, offset_two)


def solution(mesh):
    in_specs = (
        P(("rep", "tile"), None, None, None),
        P("rep", None),
        P("rep"),
        P("rep"),
        P(),
        P(),
        P(),
        P(),
        P(),
        P(),
        P(),
        P(),
    )
    out_specs = P(("rep", "tile"), None, None, None)

    def body(*args):
        return shards(*args, size=mesh.shape[AXIS])

    return jax.shard_map(body, mesh=mesh, in_specs=in_specs, out_specs=out_specs, check_vma=False)
```
